512 devices in a mesh: aux: 16 (over x_lo, z), pair: 32 (over y, x_hi, core).
Axes of the slice: x: 4 (x_hi: 2, x_lo: 2; x = x_hi * 2 + x_lo), y: 8, z: 8, core: 2. Of those that a mesh axis runs over, the one named last changes fastest.
Arguments:
- metric: bfloat16 [4096, 4096], P('aux', 'pair'), may hold values from -0.09375 to 0.09375
- amplitudes: bfloat16 [4096, 16384], P('aux', 'pair'), may hold values from -0.59765625 to 0.59765625
- virt_coef: bfloat16 [1024, 1280], replicated, may hold values from -1.5 to 1.5
Outputs:
- density: float32 [4096, 4096], P('aux', 'pair')
- fitted_ao: bfloat16 [4096, 20480], P(('aux', 'pair'))
The draws below stay inside these ranges and needn't reach their ends.
All inputs are finite; a program needn't handle non-finite values.
Results may differ from the reference program's by a relative error of at most 0.012.
Values may be sent and summed in bfloat16 or wider, within the bound.
No kernel may reach another device: no remote copies, remote signals or barrier semaphores. Data moves between devices by JAX's collectives and lax.ppermute only.
A program may use at most 64 MiB of HBM per device.

```python
import jax
import jax.numpy as jnp
from jax import lax

P_SIZE = 4096
V = 1024
AO = 1280
OCC = 16
PAIRS = 16384


def raised(drawn, key, source, target, blocks, factor):
    owner, partner = [(jnp.arange(drawn.shape[position]) // (drawn.shape[position] // blocks)).reshape([-1 if axis == position else 1 for axis in range(drawn.ndim)]) for position in (source, target)]
    chosen = jax.random.permutation(key, blocks)[partner]
    strong = (owner == chosen) | (owner == (partner + blocks // 2) % blocks)
    return jnp.where(strong, factor * drawn, drawn)


def block_levels(key, shape, cuts, least, top_value):
    factor_of, own = 1.0, jax.random.fold_in(key, 6)
    for axis_at, parts in cuts:
        heights = jnp.exp(jax.random.uniform(jax.random.fold_in(own, axis_at), (parts,), jnp.float32, least / len(cuts), top_value / len(cuts)))
        factor_of = factor_of * jnp.repeat(heights, shape[axis_at] // parts).reshape([-1 if axis == axis_at else 1 for axis in range(len(shape))])
    return factor_of


def bell_draw(own_key, dims, deviation, limit, cuts=(), dtype=jnp.bfloat16):
    gain = block_levels(own_key, dims, cuts, -0.22, 0.18) if cuts else 1.0
    array = jax.random.normal(own_key, dims, jnp.float32) * deviation * gain
    return jnp.minimum(jnp.maximum(array, -limit), limit).astype(dtype)


def heavy_noise(stream_key, shape, width, reach, pieces, heavy, kind=jnp.bfloat16):
    entries = width * jax.random.normal(stream_key, shape, jnp.float32)
    if pieces:
        entries = entries * block_levels(stream_key, shape, pieces, -0.22, 0.18)
    return jnp.clip(raised(entries, jax.random.fold_in(stream_key, 3), *heavy), -reach, reach).astype(kind)


def setup_inputs(seed: int = 0) -> dict:
    streams_of = jax.random.split(jax.random.key(seed), 4)
    return {
        "metric": bell_draw(streams_of[0], (P_SIZE, P_SIZE), P_SIZE ** -0.5, 0.09375, ((0, 16), (1, 32))),
        "amplitudes": heavy_noise(streams_of[1], (P_SIZE, PAIRS), 0.1, 0.59765625, ((0, 16), (1, 32)), (1, 0, 32, 2.75)),
        "virt_coef": bell_draw(streams_of[2], (V, AO), (V // 64) ** -0.5, 1.5),
    }


def reference(metric, amplitudes, virt_coef):
    fitted = jnp.dot(metric, amplitudes, preferred_element_type=jnp.float32).astype(jnp.bfloat16)
    density = lax.dot_general(fitted, amplitudes, (((1,), (1,)), ((), ())), preferred_element_type=jnp.float32)
    blocks = fitted.reshape(P_SIZE * OCC, V)
    fitted_ao = jnp.dot(blocks, virt_coef, preferred_element_type=jnp.float32).astype(jnp.bfloat16)
    return density, fitted_ao.reshape(P_SIZE, OCC * AO)
```

```python
import functools

import jax
import jax.numpy as jnp
from jax import lax
from jax.experimental import pallas as pl
from jax.experimental.pallas import tpu as pltpu
from jax.sharding import Mesh
from jax.sharding import PartitionSpec as P

AUX = ("xl", "z")
PAIR = ("y", "xh", "c")
ALL = AUX + PAIR
CHUNKS = 1
VMEM = pl.BlockSpec(memory_space=pltpu.VMEM)


def shifted(x, axis, by):
    n = lax.axis_size(axis)
    return lax.ppermute(x, axis, [(i, (i + by) % n) for i in range(n)])


def exchange(x, axes):
    return lax.all_to_all(x, axes, split_axis=0, concat_axis=0, tiled=True)


def ring_blocks(x):
    n = lax.axis_size("z")
    half = x.shape[1] // 2
    right, left = x, x
    blocks, offsets = [x], [0]
    for s in range(1, n // 2):
        right, left = shifted(right, "z", 1), shifted(left, "z", -1)
        blocks += [right, left]
        offsets += [n - s, s]
    far = [shifted(right[:, :half], "z", 1), shifted(left[:, half:], "z", -1)]
    return blocks, offsets, far, n // 2


def loaded(refs, offsets, far_refs, far_offset):
    values = [(o, r[...]) for o, r in zip(offsets, refs)]
    far = jnp.concatenate([r[...] for r in far_refs], axis=1)
    return values + [(far_offset, far)]


def fitted_kernel(offsets, far_offset, chunks, own_ref, other_ref, *refs):
    count = len(offsets)
    blocks = loaded(refs[:count], offsets, refs[count : count + 2], far_offset)
    wide_refs = refs[count + 2 : count + 2 + chunks]
    narrow_refs = refs[count + 2 + chunks :]
    n = 8
    z, c = lax.axis_index("z"), lax.axis_index("c")
    half = own_ref.shape[-1]
    right = []
    for i, (_, block) in enumerate(blocks):
        first, second = block[:half], block[half:]
        right += [jnp.where(c == 0, first, second), jnp.where(c == 0, second, first)]
    rhs = jnp.concatenate(right, axis=0)
    for h in range(2):
        left = []
        for offset, _ in blocks:
            at = lax.rem(z + offset, n)
            far, near = lax.rem(at, 2), lax.div(at, 2)
            left += [own_ref[h, far, near], other_ref[h, far, near]]
        lhs = jnp.concatenate(left, axis=1)
        out = jnp.dot(lhs, rhs, preferred_element_type=jnp.float32)
        rows = out.shape[0] // chunks
        for j in range(chunks):
            part = out[j * rows : (j + 1) * rows]
            wide_refs[j][h] = part
            narrow_refs[j][h] = part.astype(jnp.bfloat16)


def density_kernel(offsets, far_offset, wide_ref, arrived_ref, *refs):
    count = len(offsets)
    blocks = loaded(refs[:count], offsets, refs[count : count + 2], far_offset)
    keep_ref, send_ref, fitted_ref = refs[count + 2 :]
    n = 8
    z, c, xl = lax.axis_index("z"), lax.axis_index("c"), lax.axis_index("xl")
    fitted_ref[...] = (wide_ref[xl] + arrived_ref[xl].astype(jnp.float32)).astype(jnp.bfloat16)
    rows = wide_ref.shape[1]
    whole = (wide_ref[...] + arrived_ref[...].astype(jnp.float32)).astype(jnp.bfloat16)
    lhs = whole.reshape(2 * rows, whole.shape[2])
    for offset, block in blocks:
        at = lax.rem(z + offset, n)
        far, near = lax.rem(at, 2), lax.div(at, 2)
        out = lax.dot_general(
            lhs, block, (((1,), (1,)), ((), ())), preferred_element_type=jnp.float32
        ).astype(jnp.bfloat16)
        half = out.shape[1] // 2
        first, second = out[:, :half], out[:, half:]
        keep = jnp.where(c == 0, first, second)
        send = jnp.where(c == 0, second, first)
        for h in range(2):
            keep_ref[h, far, near] = keep[h * rows : (h + 1) * rows]
            send_ref[h, far, near] = send[h * rows : (h + 1) * rows]


def shards(metric, amplitudes, virt_coef):
    xl = lax.axis_index("xl")
    ys = exchange(jnp.broadcast_to(metric, (8, *metric.shape)), "y")
    ys = ys.reshape(2, 1, 4, *metric.shape)
    wanted = jnp.broadcast_to(ys, (2, 2, 4, *metric.shape))
    own = exchange(wanted.reshape(4, 4, *metric.shape), ("xl", "xh"))
    own = own.reshape(2, 2, 4, *metric.shape)
    other = shifted(own, "c", 1)

    blocks, offsets, far, far_offset = ring_blocks(amplitudes)
    rows, cols = metric.shape[0], amplitudes.shape[1]
    part = rows // CHUNKS
    outs = pl.pallas_call(
        functools.partial(fitted_kernel, offsets, far_offset, CHUNKS),
        in_specs=[VMEM] * (2 + len(blocks) + 2),
        out_specs=[VMEM] * (2 * CHUNKS),
        out_shape=[jax.ShapeDtypeStruct((2, part, cols), jnp.float32)] * CHUNKS
        + [jax.ShapeDtypeStruct((2, part, cols), jnp.bfloat16)] * CHUNKS,
    )(own, other, *blocks, *far)
    wides, narrows = outs[:CHUNKS], outs[CHUNKS:]

    results, fitteds = [], []
    for wide, narrow in zip(wides, narrows):
        arrived = shifted(narrow, "xl", 1)
        keep, send, fitted = pl.pallas_call(
            functools.partial(density_kernel, offsets, far_offset),
            in_specs=[VMEM] * (2 + len(blocks) + 2),
            out_specs=[VMEM] * 3,
            out_shape=[jax.ShapeDtypeStruct((2, 2, 4, part, 128), jnp.bfloat16)] * 2
            + [jax.ShapeDtypeStruct((part, cols), jnp.bfloat16)],
        )(wide, arrived, *blocks, *far)
        fitteds.append(fitted)
        got = shifted(send, "c", 1)
        both = (keep.astype(jnp.float32) + got.astype(jnp.float32)).astype(jnp.bfloat16)
        xs = exchange(both.reshape(4, 4, part, 128), ("xl", "xh")).reshape(2, 2, 4, part, 128)
        xs = jnp.sum(xs.astype(jnp.float32), axis=1).astype(jnp.bfloat16)
        ysum = exchange(xs.reshape(8, part, 128), "y")
        results.append(jnp.sum(ysum.astype(jnp.float32), axis=0))
    density = results[0] if CHUNKS == 1 else jnp.concatenate(results, axis=0)

    fitted = fitteds[0] if CHUNKS == 1 else jnp.concatenate(fitteds, axis=0)
    got = exchange(fitted.reshape(32, 8, cols), PAIR)
    got = got.reshape(16, 2, 8, cols).transpose(0, 2, 1, 3).reshape(128, 2 * cols)
    ao = jnp.dot(got, virt_coef, preferred_element_type=jnp.float32).astype(jnp.bfloat16)
    ao_count = virt_coef.shape[1]
    ao = ao.reshape(16, 8, ao_count).transpose(1, 0, 2).reshape(8, 16 * ao_count)
    return density, ao


def solution(mesh):
    split = Mesh(mesh.devices.reshape(2, 8, 8, 2, 2), ALL)
    return jax.shard_map(
        shards,
        mesh=split,
        in_specs=(P(AUX, PAIR), P(AUX, PAIR), P()),
        out_specs=(P(AUX, PAIR), P(ALL, None)),
        check_vma=False,
    )
```

```python
import functools

import jax
import jax.numpy as jnp
from jax import lax
from jax.experimental import pallas as pl
from jax.experimental.pallas import tpu as pltpu
from jax.sharding import Mesh
from jax.sharding import PartitionSpec as P


AUX = ("xl", "z")
PAIR = ("y", "xh", "c")
ALL = AUX + PAIR
CHUNKS = 1
VMEM = pl.BlockSpec(memory_space=pltpu.VMEM)
PARAMS = pltpu.CompilerParams(vmem_limit_bytes=24 * 1024 * 1024)


def in_vmem(kernel, outs, *args):
    args = [pltpu.with_memory_space_constraint(a, pltpu.VMEM) for a in args]
    return pl.pallas_call(
        kernel,
        in_specs=[VMEM] * len(args),
        out_specs=[VMEM] * len(outs),
        out_shape=[pltpu.VMEM(shape, dtype) for shape, dtype in outs],
        compiler_params=PARAMS,
    )(*args)


def shifted(x, axis, by):
    n = lax.axis_size(axis)
    return lax.ppermute(x, axis, [(i, (i + by) % n) for i in range(n)])


def exchange(x, axes):
    return lax.all_to_all(x, axes, split_axis=0, concat_axis=0, tiled=True)


def ring_blocks(x):
    n = lax.axis_size("z")
    half = x.shape[1] // 2
    right, left = x, x
    blocks, offsets = [x], [0]
    for s in range(1, n // 2):
        right, left = shifted(right, "z", 1), shifted(left, "z", -1)
        blocks += [right, left]
        offsets += [n - s, s]
    far = [shifted(right[:, :half], "z", 1), shifted(left[:, half:], "z", -1)]
    return blocks, offsets, far, n // 2


def loaded(refs, offsets, far_refs, far_offset):
    values = [(o, r[...]) for o, r in zip(offsets, refs)]
    far = jnp.concatenate([r[...] for r in far_refs], axis=1)
    return values + [(far_offset, far)]


def fitted_kernel(offsets, far_offset, chunks, own_ref, other_ref, *refs):
    count = len(offsets)
    blocks = loaded(refs[:count], offsets, refs[count : count + 2], far_offset)
    wide_refs = refs[count + 2 : count + 2 + chunks]
    narrow_refs = refs[count + 2 + chunks :]
    n = 8
    z, c = lax.axis_index("z"), lax.axis_index("c")
    half = own_ref.shape[-1]
    right = []
    for _, block in blocks:
        first, second = block[:half], block[half:]
        right += [jnp.where(c == 0, first, second), jnp.where(c == 0, second, first)]
    rhs = jnp.concatenate(right, axis=0)
    for h in range(2):
        left = []
        for offset, _ in blocks:
            at = lax.rem(z + offset, n)
            far, near = lax.rem(at, 2), lax.div(at, 2)
            left += [own_ref[h, far, near], other_ref[h, far, near]]
        lhs = jnp.concatenate(left, axis=1)
        out = jnp.dot(lhs, rhs, preferred_element_type=jnp.float32)
        rows = out.shape[0] // chunks
        for j in range(chunks):
            part = out[j * rows : (j + 1) * rows]
            wide_refs[j][h] = part
            narrow_refs[j][h] = part.astype(jnp.bfloat16)


def join_kernel(wide_ref, arrived_ref, whole_ref, own_ref):
    xl = lax.axis_index("xl")
    rows = wide_ref.shape[1]
    for h in range(2):
        whole = wide_ref[h] + arrived_ref[h].astype(jnp.float32)
        whole_ref[h * rows : (h + 1) * rows] = whole.astype(jnp.bfloat16)
    start = pl.multiple_of(xl * rows, rows)
    own_ref[...] = whole_ref[pl.ds(start, rows)]


def density_kernel(offsets, far_offset, whole_ref, *refs):
    count = len(offsets)
    blocks = loaded(refs[:count], offsets, refs[count : count + 2], far_offset)
    keep_ref, send_ref = refs[count + 2 :]
    n = 8
    z, c = lax.axis_index("z"), lax.axis_index("c")
    x = 2 * lax.axis_index("xh") + lax.axis_index("xl")
    lhs = whole_ref[...]
    rows = lhs.shape[0] // 2
    for offset, block in blocks:
        at = lax.rem(z + offset, n)
        far, near = lax.rem(at, 2), lax.div(at, 2)
        out = lax.dot_general(
            lhs, block, (((1,), (1,)), ((), ())), preferred_element_type=jnp.float32
        ).astype(jnp.bfloat16)
        half = out.shape[1] // 2
        first, second = out[:, :half], out[:, half:]
        keep = jnp.where(c == 0, first, second)
        send = jnp.where(c == 0, second, first)
        for h in range(2):
            slot = lax.rem(2 * far + h + 4 - x, 4)
            keep_ref[slot, near] = keep[h * rows : (h + 1) * rows]
            send_ref[slot, near] = send[h * rows : (h + 1) * rows]


def add_kernel(count, *refs):
    keeps, gots, outs = refs[:count], refs[count : 2 * count], refs[2 * count :]
    part = keeps[0].shape[2]
    for j in range(count):
        for s, out in enumerate(outs):
            both = keeps[j][s].astype(jnp.float32) + gots[j][s].astype(jnp.float32)
            out[:, j * part : (j + 1) * part] = both.astype(jnp.bfloat16)


def half_sum_kernel(here_ref, far_ref, left_ref, right_ref, out_ref):
    xl = lax.axis_index("xl")
    ours = here_ref[...].astype(jnp.float32) + far_ref[...].astype(jnp.float32)
    theirs = left_ref[...].astype(jnp.float32) + right_ref[...].astype(jnp.float32)
    n = here_ref.shape[0]
    out_ref[pl.ds(xl * n, n)] = ours.astype(jnp.bfloat16)
    out_ref[pl.ds((1 - xl) * n, n)] = theirs.astype(jnp.bfloat16)


def ao_kernel(got_ref, coef_ref, out_ref):
    n, rows, _ = got_ref.shape
    both = [
        jnp.concatenate([got_ref[2 * i + c].astype(jnp.float32) for i in range(n // 2)], axis=0)
        for c in range(2)
    ]
    lhs = jnp.concatenate(both, axis=1).astype(jnp.bfloat16)
    out = jnp.dot(lhs, coef_ref[...], preferred_element_type=jnp.float32)
    count = out.shape[1]
    for i in range(n // 2):
        part = out[i * rows : (i + 1) * rows].astype(jnp.bfloat16)
        out_ref[:, i * count : (i + 1) * count] = part


def work(metric, amplitudes, virt_coef):
    ys = exchange(jnp.broadcast_to(metric, (8, *metric.shape)), "y")
    ys = ys.reshape(2, 1, 4, *metric.shape)
    wanted = jnp.broadcast_to(ys, (2, 2, 4, *metric.shape))
    own = exchange(wanted.reshape(4, 4, *metric.shape), ("xl", "xh"))
    own = own.reshape(2, 2, 4, *metric.shape)
    other = shifted(own, "c", 1)

    blocks, offsets, far, far_offset = ring_blocks(amplitudes)
    rows, cols = metric.shape[0], amplitudes.shape[1]
    part = rows // CHUNKS
    f32, bf16 = jnp.float32, jnp.bfloat16
    outs = in_vmem(
        functools.partial(fitted_kernel, offsets, far_offset, CHUNKS),
        [((2, part, cols), f32)] * CHUNKS + [((2, part, cols), bf16)] * CHUNKS,
        own, other, *blocks, *far,
    )
    wides, narrows = outs[:CHUNKS], outs[CHUNKS:]

    keeps, gots, fitteds = [], [], []
    for wide, narrow in zip(wides, narrows):
        arrived = shifted(narrow, "xl", 1)
        whole, mine = in_vmem(
            join_kernel, [((2 * part, cols), bf16), ((part, cols), bf16)], wide, arrived
        )
        fitteds.append(mine)
        keep, send = in_vmem(
            functools.partial(density_kernel, offsets, far_offset),
            [((4, 4, part, 128), bf16)] * 2,
            whole, *blocks, *far,
        )
        keeps.append(keep)
        gots.append(shifted(send, "c", 1))

    slots = in_vmem(
        functools.partial(add_kernel, CHUNKS), [((4, rows, 128), bf16)] * 4, *keeps, *gots
    )

    def sent(s):
        at = lambda x: (x % 2) * 2 + x // 2
        return lax.ppermute(slots[s], ("xl", "xh"), [(at(x), at((x + s) % 4)) for x in range(4)])

    arrived = [sent(s) for s in (2, 1, 3)]
    (xs,) = in_vmem(half_sum_kernel, [((8, rows, 128), bf16)], slots[0], *arrived)
    ysum = exchange(xs, "y")
    density = jnp.sum(ysum.astype(f32), axis=0)

    fitted = fitteds[0] if CHUNKS == 1 else jnp.concatenate(fitteds, axis=0)
    got = exchange(fitted.reshape(32, 8, cols), PAIR)
    ao_count = virt_coef.shape[1]
    ao = pl.pallas_call(
        ao_kernel,
        in_specs=[VMEM] * 2,
        out_specs=VMEM,
        out_shape=jax.ShapeDtypeStruct((8, 16 * ao_count), bf16),
        compiler_params=PARAMS,
    )(got, virt_coef)
    return density, ao


def solution(mesh):
    split = Mesh(mesh.devices.reshape(2, 8, 8, 2, 2), ALL)
    return jax.shard_map(
        work,
        mesh=split,
        in_specs=(P(AUX, PAIR), P(AUX, PAIR), P()),
        out_specs=(P(AUX, PAIR), P(ALL, None)),
        check_vma=False,
    )
```

```python
import functools

import jax
import jax.numpy as jnp
from jax import lax
from jax.experimental import pallas as pl
from jax.experimental.pallas import tpu as pltpu
from jax.sharding import Mesh
from jax.sharding import PartitionSpec as P


AUX = ("xl", "z")
PAIR = ("y", "xh", "c")
ALL = AUX + PAIR
VMEM = pl.BlockSpec(memory_space=pltpu.VMEM)
PARAMS = pltpu.CompilerParams(vmem_limit_bytes=24 * 1024 * 1024)
F32, BF16 = jnp.float32, jnp.bfloat16


def in_vmem(kernel, outs, *args):
    args = [pltpu.with_memory_space_constraint(a, pltpu.VMEM) for a in args]
    return pl.pallas_call(
        kernel,
        in_specs=[VMEM] * len(args),
        out_specs=[VMEM] * len(outs),
        out_shape=[pltpu.VMEM(shape, dtype) for shape, dtype in outs],
        compiler_params=PARAMS,
    )(*args)


def shifted(x, axis, by):
    n = lax.axis_size(axis)
    return lax.ppermute(x, axis, [(i, (i + by) % n) for i in range(n)])


def shifted_x(x, by):
    at = lambda i: (i % 2) * 2 + i // 2
    return lax.ppermute(x, ("xl", "xh"), [(at(i), at((i + by) % 4)) for i in range(4)])


def exchange(x, axes):
    return lax.all_to_all(x, axes, split_axis=0, concat_axis=0, tiled=True)


def ring_blocks(x):
    n = lax.axis_size("z")
    half = x.shape[1] // 2
    right, left = x, x
    blocks, offsets = [x], [0]
    for s in range(1, n // 2):
        right, left = shifted(right, "z", 1), shifted(left, "z", -1)
        blocks += [right, left]
        offsets += [n - s, s]
    far = [shifted(right[:, :half], "z", 1), shifted(left[:, half:], "z", -1)]
    return blocks + far, offsets + [n // 2]


def values_of(refs):
    far = jnp.concatenate([refs[-2][...], refs[-1][...]], axis=1)
    return [r[...] for r in refs[:-2]] + [far]


def place(offset):
    at = lax.rem(lax.axis_index("z") + offset, 8)
    return lax.rem(at, 2), lax.div(at, 2)


def pack_kernel(amp_ref, got_ref, out_ref):
    rows, cols = got_ref.shape
    c = lax.axis_index("c")
    out_ref[:, :cols] = amp_ref[pl.ds(pl.multiple_of(c * rows, rows), rows)]
    out_ref[:, cols:] = got_ref[...]


def fitted_kernel(offsets, metric_ref, *refs):
    blocks = values_of(refs[:-2])
    keep_ref, send_ref = refs[-2:]
    rhs = jnp.concatenate(blocks, axis=0)
    cols = keep_ref.shape[2]
    for h in range(2):
        lhs = jnp.concatenate([metric_ref[(h, *place(o))] for o in offsets], axis=1)
        out = jnp.dot(lhs, rhs, preferred_element_type=F32)
        keep_ref[h] = out[:, :cols]
        send_ref[h] = out[:, cols:].astype(BF16)


def add_kernel(keep_ref, got_ref, own_ref, other_ref):
    xl = lax.axis_index("xl")
    own_ref[...] = keep_ref[xl] + got_ref[xl].astype(F32)
    other_ref[...] = (keep_ref[1 - xl] + got_ref[1 - xl].astype(F32)).astype(BF16)


def join_kernel(own_ref, arrived_ref, out_ref):
    out_ref[...] = (own_ref[...] + arrived_ref[...].astype(F32)).astype(BF16)


def density_kernel(offsets, own_ref, own_next_ref, other_ref, other_next_ref, *refs):
    blocks = values_of(refs[:-4])
    slots = refs[-4:]
    xl = lax.axis_index("xl")
    x = 2 * lax.axis_index("xh") + xl
    own = jnp.concatenate([own_ref[...], own_next_ref[...]], axis=1)
    other = jnp.concatenate([other_ref[...], other_next_ref[...]], axis=1)
    lhs = jnp.concatenate([own, other], axis=0)
    rows, width = own.shape[0], blocks[0].shape[0]
    for i in range(0, len(blocks), 2):
        rhs = jnp.concatenate(blocks[i : i + 2], axis=0)
        out = lax.dot_general(
            lhs, rhs, (((1,), (1,)), ((), ())), preferred_element_type=F32
        ).astype(BF16)
        for j in range(2):
            far, near = place(offsets[i + j])
            cols = slice(j * width, (j + 1) * width)
            same = far == lax.axis_index("xh")
            mine, theirs = out[:rows, cols], out[rows:, cols]

            @pl.when(same)
            def _():
                slots[0][near] = mine

            @pl.when(jnp.logical_not(same))
            def _():
                slots[2][near] = mine

            next_one = lax.rem(2 * far + (1 - xl) + 4 - x, 4) == 1

            @pl.when(next_one)
            def _():
                slots[1][near] = theirs

            @pl.when(jnp.logical_not(next_one))
            def _():
                slots[3][near] = theirs


def half_sum_kernel(here_ref, far_ref, left_ref, right_ref, out_ref):
    xl = lax.axis_index("xl")
    n = here_ref.shape[0]
    ours = here_ref[...].astype(F32) + far_ref[...].astype(F32)
    theirs = left_ref[...].astype(F32) + right_ref[...].astype(F32)
    out_ref[pl.ds(xl * n, n)] = ours.astype(BF16)
    out_ref[pl.ds((1 - xl) * n, n)] = theirs.astype(BF16)


def ao_kernel(got_ref, coef_ref, out_ref):
    n, rows, _ = got_ref.shape
    both = [
        jnp.concatenate([got_ref[2 * i + c].astype(F32) for i in range(n // 2)], axis=0)
        for c in range(2)
    ]
    lhs = jnp.concatenate(both, axis=1).astype(BF16)
    out = jnp.dot(lhs, coef_ref[...], preferred_element_type=F32)
    count = out.shape[1]
    for i in range(n // 2):
        part = out[i * rows : (i + 1) * rows].astype(BF16)
        out_ref[:, i * count : (i + 1) * count] = part


def work(metric, amplitudes, virt_coef):
    rows, cols = amplitudes.shape
    c = lax.axis_index("c")
    ys = exchange(jnp.broadcast_to(metric, (8, *metric.shape)), "y")
    ys = ys.reshape(2, 1, 4, *metric.shape)
    wanted = jnp.broadcast_to(ys, (2, 2, 4, *metric.shape))
    part = exchange(wanted.reshape(4, 4, *metric.shape), ("xl", "xh"))
    part = part.reshape(2, 2, 4, *metric.shape)

    half = rows // 2
    away = lax.dynamic_slice_in_dim(amplitudes, (1 - c) * half, half, 0)
    got = shifted(away, "c", 1)
    (packed,) = in_vmem(pack_kernel, [((half, 2 * cols), BF16)], amplitudes, got)
    blocks, offsets = ring_blocks(packed)

    keep, send = in_vmem(
        functools.partial(fitted_kernel, offsets),
        [((2, rows, cols), F32), ((2, rows, cols), BF16)],
        part, *blocks,
    )
    got = shifted(send, "c", 1)
    own, away = in_vmem(add_kernel, [((rows, cols), F32), ((rows, cols), BF16)], keep, got)
    arrived = shifted(away, "xl", 1)
    (fitted,) = in_vmem(join_kernel, [((rows, cols), BF16)], own, arrived)
    other = shifted(fitted, "xl", 1)
    fitted_next = shifted(fitted, "c", 1)
    other_next = shifted(other, "c", 1)
    slots = in_vmem(
        functools.partial(density_kernel, offsets),
        [((4, rows, half), BF16)] * 4,
        fitted, fitted_next, other, other_next, *blocks,
    )
    arrived = [shifted_x(slots[s], s) for s in (2, 1, 3)]
    (xs,) = in_vmem(half_sum_kernel, [((8, rows, half), BF16)], slots[0], *arrived)
    ysum = exchange(xs, "y")
    density = jnp.sum(ysum.astype(F32), axis=0)

    got = exchange(fitted.reshape(32, 8, cols), PAIR)
    ao_count = virt_coef.shape[1]
    ao = pl.pallas_call(
        ao_kernel,
        in_specs=[VMEM] * 2,
        out_specs=VMEM,
        out_shape=jax.ShapeDtypeStruct((8, 16 * ao_count), BF16),
        compiler_params=PARAMS,
    )(got, virt_coef)
    return density, ao


def solution(mesh):
    split = Mesh(mesh.devices.reshape(2, 8, 8, 2, 2), ALL)
    return jax.shard_map(
        work,
        mesh=split,
        in_specs=(P(AUX, PAIR), P(AUX, PAIR), P()),
        out_specs=(P(AUX, PAIR), P(ALL, None)),
        check_vma=False,
    )
```

```python
import functools

import jax
import jax.numpy as jnp
from jax import lax
from jax.experimental import pallas as pl
from jax.experimental.pallas import tpu as pltpu
from jax.sharding import Mesh
from jax.sharding import PartitionSpec as P


AUX = ("xl", "z")
PAIR = ("y", "xh", "c")
ALL = AUX + PAIR
VMEM = pl.BlockSpec(memory_space=pltpu.VMEM)
PARAMS = pltpu.CompilerParams(vmem_limit_bytes=24 * 1024 * 1024)
F32, BF16 = jnp.float32, jnp.bfloat16


def in_vmem(kernel, outs, *args):
    args = [pltpu.with_memory_space_constraint(a, pltpu.VMEM) for a in args]
    return pl.pallas_call(
        kernel,
        in_specs=[VMEM] * len(args),
        out_specs=[VMEM] * len(outs),
        out_shape=[pltpu.VMEM(shape, dtype) for shape, dtype in outs],
        compiler_params=PARAMS,
    )(*args)


def shifted(x, axis, by):
    n = lax.axis_size(axis)
    return lax.ppermute(x, axis, [(i, (i + by) % n) for i in range(n)])


def exchange(x, axes):
    return lax.all_to_all(x, axes, split_axis=0, concat_axis=0, tiled=True)


def ring_blocks(x):
    n = lax.axis_size("z")
    half = x.shape[1] // 2
    right, left = x, x
    blocks, offsets = [x], [0]
    for s in range(1, n // 2):
        right, left = shifted(right, "z", 1), shifted(left, "z", -1)
        blocks += [right, left]
        offsets += [n - s, s]
    far = [shifted(right[:, :half], "z", 1), shifted(left[:, half:], "z", -1)]
    return blocks + far, offsets + [n // 2]


def values_of(refs):
    far = jnp.concatenate([refs[-2][...], refs[-1][...]], axis=1)
    return [r[...] for r in refs[:-2]] + [far]


def place(offset):
    at = lax.rem(lax.axis_index("z") + offset, 8)
    return lax.rem(at, 2), lax.div(at, 2)


def pack_kernel(amp_ref, got_ref, out_ref):
    rows, cols = got_ref.shape
    c = lax.axis_index("c")
    out_ref[:, :cols] = amp_ref[pl.ds(pl.multiple_of(c * rows, rows), rows)]
    out_ref[:, cols:] = got_ref[...]


def fitted_kernel(offsets, metric_ref, *refs):
    blocks = values_of(refs[:-2])
    keep_ref, send_ref = refs[-2:]
    rhs = jnp.concatenate(blocks, axis=0)
    cols = keep_ref.shape[2]
    for h in range(2):
        lhs = jnp.concatenate([metric_ref[(h, *place(o))] for o in offsets], axis=1)
        out = jnp.dot(lhs, rhs, preferred_element_type=F32)
        keep_ref[h] = out[:, :cols]
        send_ref[h] = out[:, cols:].astype(BF16)


def add_kernel(keep_ref, got_ref, own_ref, other_ref):
    xl = lax.axis_index("xl")
    own_ref[...] = keep_ref[xl] + got_ref[xl].astype(F32)
    other_ref[...] = (keep_ref[1 - xl] + got_ref[1 - xl].astype(F32)).astype(BF16)


def join_kernel(own_ref, arrived_ref, out_ref):
    out_ref[...] = (own_ref[...] + arrived_ref[...].astype(F32)).astype(BF16)


def density_kernel(offsets, own_ref, own_next_ref, other_ref, other_next_ref, *refs):
    blocks = values_of(refs[:-1])
    out_ref = refs[-1]
    xl = lax.axis_index("xl")
    own = jnp.concatenate([own_ref[...], own_next_ref[...]], axis=1)
    other = jnp.concatenate([other_ref[...], other_next_ref[...]], axis=1)
    lhs = jnp.concatenate([own, other], axis=0)
    rows, width = own.shape[0], blocks[0].shape[0]
    for i in range(0, len(blocks), 2):
        rhs = jnp.concatenate(blocks[i : i + 2], axis=0)
        out = lax.dot_general(
            lhs, rhs, (((1,), (1,)), ((), ())), preferred_element_type=F32
        ).astype(BF16)
        for j in range(2):
            far, near = place(offsets[i + j])
            cols = slice(j * width, (j + 1) * width)
            out_ref[2 * xl + far, near] = out[:rows, cols]
            out_ref[2 * (1 - xl) + far, near] = out[rows:, cols]


def half_sum_kernel(in_ref, out_ref):
    n = in_ref.shape[1]
    for h in range(2):
        both = in_ref[2 * h].astype(F32) + in_ref[2 * h + 1].astype(F32)
        out_ref[h * n : (h + 1) * n] = both.astype(BF16)


def ao_kernel(got_ref, coef_ref, out_ref):
    n, rows, _ = got_ref.shape
    both = [
        jnp.concatenate([got_ref[2 * i + c].astype(F32) for i in range(n // 2)], axis=0)
        for c in range(2)
    ]
    lhs = jnp.concatenate(both, axis=1).astype(BF16)
    out = jnp.dot(lhs, coef_ref[...], preferred_element_type=F32)
    count = out.shape[1]
    for i in range(n // 2):
        part = out[i * rows : (i + 1) * rows].astype(BF16)
        out_ref[:, i * count : (i + 1) * count] = part


def work(metric, amplitudes, virt_coef):
    rows, cols = amplitudes.shape
    c = lax.axis_index("c")
    ys = exchange(jnp.broadcast_to(metric, (8, *metric.shape)), "y")
    ys = ys.reshape(2, 1, 4, *metric.shape)
    wanted = jnp.broadcast_to(ys, (2, 2, 4, *metric.shape))
    part = exchange(wanted.reshape(4, 4, *metric.shape), ("xl", "xh"))
    part = part.reshape(2, 2, 4, *metric.shape)

    half = rows // 2
    away = lax.dynamic_slice_in_dim(amplitudes, (1 - c) * half, half, 0)
    got = shifted(away, "c", 1)
    (packed,) = in_vmem(pack_kernel, [((half, 2 * cols), BF16)], amplitudes, got)
    blocks, offsets = ring_blocks(packed)

    keep, send = in_vmem(
        functools.partial(fitted_kernel, offsets),
        [((2, rows, cols), F32), ((2, rows, cols), BF16)],
        part, *blocks,
    )
    got = shifted(send, "c", 1)
    own, away = in_vmem(add_kernel, [((rows, cols), F32), ((rows, cols), BF16)], keep, got)
    arrived = shifted(away, "xl", 1)
    (fitted,) = in_vmem(join_kernel, [((rows, cols), BF16)], own, arrived)
    other = shifted(fitted, "xl", 1)
    fitted_next = shifted(fitted, "c", 1)
    other_next = shifted(other, "c", 1)
    (parts,) = in_vmem(
        functools.partial(density_kernel, offsets),
        [((4, 4, rows, half), BF16)],
        fitted, fitted_next, other, other_next, *blocks,
    )
    parts = exchange(parts, ("xl", "xh"))
    (xs,) = in_vmem(half_sum_kernel, [((8, rows, half), BF16)], parts)
    ysum = exchange(xs, "y")
    density = jnp.sum(ysum.astype(F32), axis=0)

    got = exchange(fitted.reshape(32, 8, cols), PAIR)
    ao_count = virt_coef.shape[1]
    ao = pl.pallas_call(
        ao_kernel,
        in_specs=[VMEM] * 2,
        out_specs=VMEM,
        out_shape=jax.ShapeDtypeStruct((8, 16 * ao_count), BF16),
        compiler_params=PARAMS,
    )(got, virt_coef)
    return density, ao


def solution(mesh):
    split = Mesh(mesh.devices.reshape(2, 8, 8, 2, 2), ALL)
    return jax.shard_map(
        work,
        mesh=split,
        in_specs=(P(AUX, PAIR), P(AUX, PAIR), P()),
        out_specs=(P(AUX, PAIR), P(ALL, None)),
        check_vma=False,
    )
```

```python
import jax
import jax.numpy as jnp
from jax import lax
from jax.experimental import pallas as pl
from jax.experimental.pallas import tpu as pltpu
from jax.sharding import Mesh
from jax.sharding import PartitionSpec as P


AUX = ("xl", "z")
PAIR = ("y", "xh", "c")
ALL = AUX + PAIR
VMEM = pl.BlockSpec(memory_space=pltpu.VMEM)
PARAMS = pltpu.CompilerParams(vmem_limit_bytes=24 * 1024 * 1024)
F32, BF16 = jnp.float32, jnp.bfloat16


def in_vmem(kernel, outs, *args):
    args = [pltpu.with_memory_space_constraint(a, pltpu.VMEM) for a in args]
    return pl.pallas_call(
        kernel,
        in_specs=[VMEM] * len(args),
        out_specs=[VMEM] * len(outs),
        out_shape=[pltpu.VMEM(shape, dtype) for shape, dtype in outs],
        compiler_params=PARAMS,
    )(*args)


def shifted(x, axis, by):
    n = lax.axis_size(axis)
    return lax.ppermute(x, axis, [(i, (i + by) % n) for i in range(n)])


def exchange(x, axes):
    return lax.all_to_all(x, axes, split_axis=0, concat_axis=0, tiled=True)


def ring_step(x):
    n = lax.axis_size("z")
    moves = [(2 * i, 2 * ((i + 1) % n)) for i in range(n)]
    moves += [(2 * i + 1, 2 * ((i - 1) % n) + 1) for i in range(n)]
    return lax.ppermute(x, ("z", "c"), moves)


def shifted_x(x, by):
    at = lambda i: (i % 2) * 2 + i // 2
    return lax.ppermute(x, ("xl", "xh"), [(at(i), at((i + by) % 4)) for i in range(4)])


def blocks_of(refs):
    c = lax.axis_index("c")
    toward = 2 * c - 1
    blocks = [(0, refs[0][...])]
    for s in range(1, 4):
        blocks += [(toward * s, refs[s][...]), (-toward * s, refs[3 + s][...])]
    mine, got = refs[7][...], refs[8][...]
    first = jnp.where(c == 0, mine, got)
    second = jnp.where(c == 0, got, mine)
    return blocks + [(4, jnp.concatenate([first, second], axis=0))]


def place(offset):
    at = lax.rem(lax.axis_index("z") + offset + 8, 8)
    return lax.rem(at, 2), lax.div(at, 2)


def pack_kernel(amp_ref, got_ref, out_ref):
    cols = got_ref.shape[1]
    first = lax.axis_index("c") == 0
    own, got = amp_ref[...], got_ref[...]
    out_ref[:, :cols] = jnp.where(first, own, got)
    out_ref[:, cols:] = jnp.where(first, got, own)


def half_kernel(in_ref, out_ref):
    rows = out_ref.shape[0]
    out_ref[...] = in_ref[pl.ds(pl.multiple_of(lax.axis_index("c") * rows, rows), rows)]


def fitted_kernel(metric_ref, *refs):
    blocks = blocks_of(refs[:-2])
    own_ref, away_ref = refs[-2:]
    xl = lax.axis_index("xl")
    rhs = jnp.concatenate([b for _, b in blocks], axis=0)
    for h, ref in ((xl, own_ref), (1 - xl, away_ref)):
        lhs = [metric_ref[(h, *place(o), j)] for o, _ in blocks for j in range(2)]
        out = jnp.dot(jnp.concatenate(lhs, axis=1), rhs, preferred_element_type=F32)
        ref[...] = out.astype(ref.dtype)


def join_kernel(own_ref, arrived_ref, out_ref):
    out_ref[...] = (own_ref[...] + arrived_ref[...].astype(F32)).astype(BF16)


def density_kernel(own_ref, other_ref, *refs):
    blocks = blocks_of(refs[:-5])
    outs, all_ref = refs[-5:-1], refs[-1]
    xl = lax.axis_index("xl")
    x = 2 * lax.axis_index("xh") + xl
    lhs = jnp.concatenate([own_ref[...], other_ref[...]], axis=0)
    rows = own_ref.shape[0]
    for offset, block in blocks:
        out = lax.dot_general(
            lhs, block, (((1,), (1,)), ((), ())), preferred_element_type=F32
        ).astype(BF16)
        far, near = place(offset)
        half = out.shape[1] // 2
        for h, part in ((xl, out[:rows]), (1 - xl, out[rows:])):
            slot = lax.rem(2 * far + h + 4 - x, 4)
            for j in range(2):
                all_ref[slot, near, j] = part[:, j * half : (j + 1) * half]
    for s in range(4):
        outs[s][...] = all_ref[s]


def half_sum_kernel(here_ref, far_ref, left_ref, right_ref, out_ref):
    xl = lax.axis_index("xl")
    n = here_ref.shape[0]
    ours = here_ref[...].astype(F32) + far_ref[...].astype(F32)
    theirs = left_ref[...].astype(F32) + right_ref[...].astype(F32)
    out_ref[pl.ds(xl * n, n)] = ours.astype(BF16)
    out_ref[pl.ds((1 - xl) * n, n)] = theirs.astype(BF16)


def last_sum_kernel(in_ref, out_ref):
    groups, _, rows, _ = out_ref.shape
    for c in range(2):
        total = in_ref[0, c].astype(F32)
        for y in range(1, in_ref.shape[0]):
            total += in_ref[y, c].astype(F32)
        for g in range(groups):
            out_ref[g, c] = total[g * rows : (g + 1) * rows]


def ao_kernel(got_ref, coef_ref, out_ref):
    n, rows, _ = got_ref.shape
    lhs = jnp.concatenate([got_ref[i].astype(F32) for i in range(n)], axis=0).astype(BF16)
    out = jnp.dot(lhs, coef_ref[...], preferred_element_type=F32)
    count = out.shape[1]
    for i in range(n):
        part = out[i * rows : (i + 1) * rows].astype(BF16)
        out_ref[:, i * count : (i + 1) * count] = part


def work(metric, amplitudes, virt_coef):
    rows, cols = amplitudes.shape
    half, width = rows // 2, metric.shape[1]
    by_core = metric.reshape(rows // 16, 2, 8, width).swapaxes(0, 1).reshape(2, half, width)
    ys = exchange(jnp.tile(by_core, (8, 1, 1)), ("y", "c"))
    ys = ys.reshape(2, 1, 4, 2, half, width)
    wanted = jnp.broadcast_to(ys, (2, 2, 4, 2, half, width))
    part = exchange(wanted.reshape(4, 4, 2, half, width), ("xl", "xh"))
    part = part.reshape(2, 2, 4, 2, half, width)

    got = shifted(amplitudes, "c", 1)
    (packed,) = in_vmem(pack_kernel, [((rows, 2 * cols), BF16)], amplitudes, got)
    steps = [packed]
    for _ in range(1, 4):
        steps.append(ring_step(steps[-1]))
    swaps = [shifted(steps[s], "c", 1) for s in range(1, 4)]
    (farther,) = in_vmem(half_kernel, [((half, 2 * cols), BF16)], steps[3])
    far = ring_step(farther)
    blocks = steps + swaps + [far, shifted(far, "c", 1)]

    own, away = in_vmem(
        fitted_kernel, [((half, 2 * cols), F32), ((half, 2 * cols), BF16)], part, *blocks
    )
    arrived = shifted(away, "xl", 1)
    (fitted,) = in_vmem(join_kernel, [((half, 2 * cols), BF16)], own, arrived)
    other = shifted(fitted, "xl", 1)
    args = [pltpu.with_memory_space_constraint(a, pltpu.VMEM) for a in (fitted, other, *blocks)]
    piece = (4, 2, half, half)
    slots = pl.pallas_call(
        density_kernel,
        in_specs=[VMEM] * len(args),
        out_specs=[VMEM] * 4,
        out_shape=[pltpu.VMEM(piece, BF16)] * 4,
        scratch_shapes=[pltpu.VMEM((4, *piece), BF16)],
        compiler_params=PARAMS,
    )(*args)
    arrived = [shifted_x(slots[s], s) for s in (2, 1, 3)]
    (xs,) = in_vmem(half_sum_kernel, [((8, 2, half, half), BF16)], slots[0], *arrived)
    got = exchange(xs.reshape(16, half, half), ("y", "c"))
    density = pl.pallas_call(
        last_sum_kernel,
        in_specs=[VMEM],
        out_specs=VMEM,
        out_shape=jax.ShapeDtypeStruct((rows // 16, 2, 8, half), F32),
        compiler_params=PARAMS,
    )(got.reshape(8, 2, half, half))

    got = exchange(fitted.reshape(16, 8, 2 * cols), ("y", "xh"))
    ao_count = virt_coef.shape[1]
    ao = pl.pallas_call(
        ao_kernel,
        in_specs=[VMEM] * 2,
        out_specs=VMEM,
        out_shape=jax.ShapeDtypeStruct((8, 16 * ao_count), BF16),
        compiler_params=PARAMS,
    )(got, virt_coef)
    return density.reshape(rows, half), ao


def solution(mesh):
    split = Mesh(mesh.devices.reshape(2, 8, 8, 2, 2), ALL)
    return jax.shard_map(
        work,
        mesh=split,
        in_specs=(P(AUX, PAIR), P(AUX, PAIR), P()),
        out_specs=(P(AUX, PAIR), P(ALL, None)),
        check_vma=False,
    )
```

```python
import jax
import jax.numpy as jnp
from jax import lax
from jax.experimental import pallas as pl
from jax.experimental.pallas import tpu as pltpu
from jax.sharding import Mesh
from jax.sharding import PartitionSpec as P


AUX = ("xl", "z")
PAIR = ("y", "xh", "c")
ALL = AUX + PAIR
VMEM = pl.BlockSpec(memory_space=pltpu.VMEM)
PARAMS = pltpu.CompilerParams(vmem_limit_bytes=24 * 1024 * 1024)
F32, BF16 = jnp.float32, jnp.bfloat16


def in_vmem(kernel, outs, *args):
    args = [pltpu.with_memory_space_constraint(a, pltpu.VMEM) for a in args]
    return pl.pallas_call(
        kernel,
        in_specs=[VMEM] * len(args),
        out_specs=[VMEM] * len(outs),
        out_shape=[pltpu.VMEM(shape, dtype) for shape, dtype in outs],
        compiler_params=PARAMS,
    )(*args)


def shifted(x, axis, by):
    n = lax.axis_size(axis)
    return lax.ppermute(x, axis, [(i, (i + by) % n) for i in range(n)])


def exchange(x, axes):
    return lax.all_to_all(x, axes, split_axis=0, concat_axis=0, tiled=True)


def ring_step(x):
    n = lax.axis_size("z")
    moves = [(2 * i, 2 * ((i + 1) % n)) for i in range(n)]
    moves += [(2 * i + 1, 2 * ((i - 1) % n) + 1) for i in range(n)]
    return lax.ppermute(x, ("z", "c"), moves)


def shifted_x(x, by):
    at = lambda i: (i % 2) * 2 + i // 2
    return lax.ppermute(x, ("xl", "xh"), [(at(i), at((i + by) % 4)) for i in range(4)])


def blocks_of(refs):
    c = lax.axis_index("c")
    toward = 2 * c - 1
    blocks = [(0, refs[0][...])]
    for s in range(1, 4):
        blocks += [(toward * s, refs[s][...]), (-toward * s, refs[3 + s][...])]
    mine, got = refs[7][...], refs[8][...]
    first = jnp.where(c == 0, mine, got)
    second = jnp.where(c == 0, got, mine)
    return blocks + [(4, jnp.concatenate([first, second], axis=0))]


def place(offset):
    at = lax.rem(lax.axis_index("z") + offset + 8, 8)
    return lax.rem(at, 2), lax.div(at, 2)


def pack_kernel(amp_ref, got_ref, out_ref):
    cols = got_ref.shape[1]
    first = lax.axis_index("c") == 0
    own, got = amp_ref[...], got_ref[...]
    out_ref[:, :cols] = jnp.where(first, own, got)
    out_ref[:, cols:] = jnp.where(first, got, own)


def split_kernel(in_ref, out_ref):
    n, cores, rows, cols = out_ref.shape
    groups = in_ref[...].astype(F32).reshape(rows // 8, cores, 8, cols)
    for c in range(cores):
        part = groups[:, c].reshape(rows, cols).astype(BF16)
        for i in range(n):
            out_ref[i, c] = part


def half_kernel(in_ref, out_ref):
    rows = out_ref.shape[0]
    out_ref[...] = in_ref[pl.ds(pl.multiple_of(lax.axis_index("c") * rows, rows), rows)]


def fitted_kernel(metric_ref, *refs):
    blocks = blocks_of(refs[:-2])
    own_ref, away_ref = refs[-2:]
    xl = lax.axis_index("xl")
    rhs = jnp.concatenate([b for _, b in blocks], axis=0)
    for h, ref in ((xl, own_ref), (1 - xl, away_ref)):
        lhs = [metric_ref[(h, *place(o), j)] for o, _ in blocks for j in range(2)]
        out = jnp.dot(jnp.concatenate(lhs, axis=1), rhs, preferred_element_type=F32)
        ref[...] = out.astype(ref.dtype)


def join_kernel(own_ref, arrived_ref, out_ref):
    out_ref[...] = (own_ref[...] + arrived_ref[...].astype(F32)).astype(BF16)


def density_kernel(own_ref, other_ref, *refs):
    blocks = blocks_of(refs[:-5])
    outs, all_ref = refs[-5:-1], refs[-1]
    xl = lax.axis_index("xl")
    x = 2 * lax.axis_index("xh") + xl
    lhs = jnp.concatenate([own_ref[...], other_ref[...]], axis=0)
    rows = own_ref.shape[0]
    for offset, block in blocks:
        out = lax.dot_general(
            lhs, block, (((1,), (1,)), ((), ())), preferred_element_type=F32
        ).astype(BF16)
        far, near = place(offset)
        half = out.shape[1] // 2
        for h, part in ((xl, out[:rows]), (1 - xl, out[rows:])):
            slot = lax.rem(2 * far + h + 4 - x, 4)
            for j in range(2):
                all_ref[slot, near, j] = part[:, j * half : (j + 1) * half]
    for s in range(4):
        outs[s][...] = all_ref[s]


def half_sum_kernel(here_ref, far_ref, left_ref, right_ref, out_ref):
    xl = lax.axis_index("xl")
    n = here_ref.shape[0]
    ours = here_ref[...].astype(F32) + far_ref[...].astype(F32)
    theirs = left_ref[...].astype(F32) + right_ref[...].astype(F32)
    out_ref[pl.ds(xl * n, n)] = ours.astype(BF16)
    out_ref[pl.ds((1 - xl) * n, n)] = theirs.astype(BF16)


def last_sum_kernel(in_ref, out_ref):
    groups, _, rows, _ = out_ref.shape
    for c in range(2):
        total = in_ref[0, c].astype(F32)
        for y in range(1, in_ref.shape[0]):
            total += in_ref[y, c].astype(F32)
        for g in range(groups):
            out_ref[g, c] = total[g * rows : (g + 1) * rows]


def ao_kernel(got_ref, coef_ref, out_ref):
    n, rows, _ = got_ref.shape
    lhs = jnp.concatenate([got_ref[i].astype(F32) for i in range(n)], axis=0).astype(BF16)
    out = jnp.dot(lhs, coef_ref[...], preferred_element_type=F32)
    count = out.shape[1]
    for i in range(n):
        part = out[i * rows : (i + 1) * rows].astype(BF16)
        out_ref[:, i * count : (i + 1) * count] = part


def work(metric, amplitudes, virt_coef):
    rows, cols = amplitudes.shape
    half, width = rows // 2, metric.shape[1]
    by_core = pl.pallas_call(
        split_kernel,
        in_specs=[VMEM],
        out_specs=VMEM,
        out_shape=jax.ShapeDtypeStruct((8, 2, half, width), BF16),
        compiler_params=PARAMS,
    )(metric)
    ys = exchange(by_core.reshape(16, half, width), ("y", "c"))
    ys = ys.reshape(2, 1, 4, 2, half, width)
    wanted = jnp.broadcast_to(ys, (2, 2, 4, 2, half, width))
    part = exchange(wanted.reshape(4, 4, 2, half, width), ("xl", "xh"))
    part = part.reshape(2, 2, 4, 2, half, width)

    got = shifted(amplitudes, "c", 1)
    (packed,) = in_vmem(pack_kernel, [((rows, 2 * cols), BF16)], amplitudes, got)
    steps = [packed]
    for _ in range(1, 4):
        steps.append(ring_step(steps[-1]))
    swaps = [shifted(steps[s], "c", 1) for s in range(1, 4)]
    (farther,) = in_vmem(half_kernel, [((half, 2 * cols), BF16)], steps[3])
    far = ring_step(farther)
    blocks = steps + swaps + [far, shifted(far, "c", 1)]

    own, away = in_vmem(
        fitted_kernel, [((half, 2 * cols), F32), ((half, 2 * cols), BF16)], part, *blocks
    )
    arrived = shifted(away, "xl", 1)
    (fitted,) = in_vmem(join_kernel, [((half, 2 * cols), BF16)], own, arrived)
    other = shifted(fitted, "xl", 1)
    args = [pltpu.with_memory_space_constraint(a, pltpu.VMEM) for a in (fitted, other, *blocks)]
    piece = (4, 2, half, half)
    slots = pl.pallas_call(
        density_kernel,
        in_specs=[VMEM] * len(args),
        out_specs=[VMEM] * 4,
        out_shape=[pltpu.VMEM(piece, BF16)] * 4,
        scratch_shapes=[pltpu.VMEM((4, *piece), BF16)],
        compiler_params=PARAMS,
    )(*args)
    arrived = [shifted_x(slots[s], s) for s in (2, 1, 3)]
    (xs,) = in_vmem(half_sum_kernel, [((8, 2, half, half), BF16)], slots[0], *arrived)
    got = exchange(xs.reshape(16, half, half), ("y", "c"))
    density = pl.pallas_call(
        last_sum_kernel,
        in_specs=[VMEM],
        out_specs=VMEM,
        out_shape=jax.ShapeDtypeStruct((rows // 16, 2, 8, half), F32),
        compiler_params=PARAMS,
    )(got.reshape(8, 2, half, half))

    got = exchange(fitted.reshape(16, 8, 2 * cols), ("y", "xh"))
    ao_count = virt_coef.shape[1]
    ao = pl.pallas_call(
        ao_kernel,
        in_specs=[VMEM] * 2,
        out_specs=VMEM,
        out_shape=jax.ShapeDtypeStruct((8, 16 * ao_count), BF16),
        compiler_params=PARAMS,
    )(got, pltpu.with_memory_space_constraint(virt_coef, pltpu.HBM))
    return density.reshape(rows, half), ao


def solution(mesh):
    split = Mesh(mesh.devices.reshape(2, 8, 8, 2, 2), ALL)
    return jax.shard_map(
        work,
        mesh=split,
        in_specs=(P(AUX, PAIR), P(AUX, PAIR), P()),
        out_specs=(P(AUX, PAIR), P(ALL, None)),
        check_vma=False,
    )
```

```python
import jax
import jax.numpy as jnp
from jax import lax
from jax.experimental import pallas as pl
from jax.experimental.pallas import tpu as pltpu
from jax.sharding import Mesh
from jax.sharding import PartitionSpec as P


AUX = ("xl", "z")
PAIR = ("y", "xh", "c")
ALL = AUX + PAIR
VMEM = pl.BlockSpec(memory_space=pltpu.VMEM)
PARAMS = pltpu.CompilerParams(vmem_limit_bytes=24 * 1024 * 1024)
F32, BF16 = jnp.float32, jnp.bfloat16


def in_vmem(kernel, outs, *args):
    args = [pltpu.with_memory_space_constraint(a, pltpu.VMEM) for a in args]
    return pl.pallas_call(
        kernel,
        in_specs=[VMEM] * len(args),
        out_specs=[VMEM] * len(outs),
        out_shape=[pltpu.VMEM(shape, dtype) for shape, dtype in outs],
        compiler_params=PARAMS,
    )(*args)


def shifted(x, axis, by):
    n = lax.axis_size(axis)
    return lax.ppermute(x, axis, [(i, (i + by) % n) for i in range(n)])


def exchange(x, axes):
    return lax.all_to_all(x, axes, split_axis=0, concat_axis=0, tiled=True)


def ring_step(x):
    n = lax.axis_size("z")
    moves = [(2 * i, 2 * ((i + 1) % n)) for i in range(n)]
    moves += [(2 * i + 1, 2 * ((i - 1) % n) + 1) for i in range(n)]
    return lax.ppermute(x, ("z", "c"), moves)


def shifted_x(x, by):
    at = lambda i: (i % 2) * 2 + i // 2
    return lax.ppermute(x, ("xl", "xh"), [(at(i), at((i + by) % 4)) for i in range(4)])


def with_blocks(near_refs, swap_refs, bufs, sems, use):
    toward = 2 * lax.axis_index("c") - 1
    copies = [
        pltpu.make_async_copy(ref, bufs.at[i], sems.at[i]) for i, ref in enumerate(swap_refs)
    ]
    for copy in copies:
        copy.start()
    near = [(toward * s, ref[...]) for s, ref in enumerate(near_refs)]
    use(near)
    for copy in copies:
        copy.wait()
    use([(-toward * (i + 1), bufs[i]) for i in range(len(copies))])


def place(offset):
    at = lax.rem(lax.axis_index("z") + offset + 8, 8)
    return lax.rem(at, 2), lax.div(at, 2)


def pack_kernel(amp_ref, got_ref, out_ref):
    cols = got_ref.shape[1]
    first = lax.axis_index("c") == 0
    own, got = amp_ref[...], got_ref[...]
    out_ref[:, :cols] = jnp.where(first, own, got)
    out_ref[:, cols:] = jnp.where(first, got, own)


def split_kernel(in_ref, out_ref):
    n, cores, rows, cols = out_ref.shape
    groups = in_ref[...].astype(F32).reshape(rows // 8, cores, 8, cols)
    for c in range(cores):
        part = groups[:, c].reshape(rows, cols).astype(BF16)
        for i in range(n):
            out_ref[i, c] = part


def fitted_kernel(metric_ref, *refs):
    near_refs, swap_refs = refs[:5], refs[5:8]
    wide_refs, narrow_refs, (bufs, sems) = refs[8:10], refs[10:12], refs[12:]
    xl = lax.axis_index("xl")
    sums = [None, None]

    def use(blocks):
        rhs = jnp.concatenate([b for _, b in blocks], axis=0)
        for i, h in enumerate((xl, 1 - xl)):
            lhs = [metric_ref[(h, *place(o), j)] for o, _ in blocks for j in range(2)]
            out = jnp.dot(jnp.concatenate(lhs, axis=1), rhs, preferred_element_type=F32)
            sums[i] = out if sums[i] is None else sums[i] + out

    with_blocks(near_refs, swap_refs, bufs, sems, use)
    for i in range(2):
        wide_refs[i][...] = sums[i]
        narrow_refs[i][...] = sums[i].astype(BF16)


def join_kernel(own_ref, arrived_ref, out_ref):
    out_ref[...] = (own_ref[...] + arrived_ref[...].astype(F32)).astype(BF16)


def density_kernel(own_ref, other_ref, arrived_ref, *refs):
    near_refs, swap_refs, outs = refs[:5], refs[5:8], refs[8:12]
    all_ref, bufs, sems = refs[12:]
    xl = lax.axis_index("xl")
    x = 2 * lax.axis_index("xh") + xl
    other = (other_ref[...] + arrived_ref[...].astype(F32)).astype(BF16)
    lhs = jnp.concatenate([own_ref[...], other], axis=0)
    rows = own_ref.shape[0]

    def use(blocks):
        for offset, block in blocks:
            out = lax.dot_general(
                lhs, block, (((1,), (1,)), ((), ())), preferred_element_type=F32
            ).astype(BF16)
            far, near = place(offset)
            half = out.shape[1] // 2
            for h, part in ((xl, out[:rows]), (1 - xl, out[rows:])):
                slot = lax.rem(2 * far + h + 4 - x, 4)
                for j in range(2):
                    all_ref[slot, near, j] = part[:, j * half : (j + 1) * half]

    with_blocks(near_refs, swap_refs, bufs, sems, use)
    for s in range(4):
        outs[s][...] = all_ref[s]


def half_sum_kernel(here_ref, far_ref, left_ref, right_ref, out_ref):
    xl = lax.axis_index("xl")
    n = here_ref.shape[0]
    ours = here_ref[...].astype(F32) + far_ref[...].astype(F32)
    theirs = left_ref[...].astype(F32) + right_ref[...].astype(F32)
    out_ref[pl.ds(xl * n, n)] = ours.astype(BF16)
    out_ref[pl.ds((1 - xl) * n, n)] = theirs.astype(BF16)


def last_sum_kernel(in_ref, out_ref):
    groups, _, rows, _ = out_ref.shape
    for c in range(2):
        total = in_ref[0, c].astype(F32)
        for y in range(1, in_ref.shape[0]):
            total += in_ref[y, c].astype(F32)
        for g in range(groups):
            out_ref[g, c] = total[g * rows : (g + 1) * rows]


def ao_kernel(got_ref, coef_ref, out_ref):
    n, rows, _ = got_ref.shape
    lhs = jnp.concatenate([got_ref[i].astype(F32) for i in range(n)], axis=0).astype(BF16)
    out = jnp.dot(lhs, coef_ref[...], preferred_element_type=F32)
    count = out.shape[1]
    for i in range(n):
        part = out[i * rows : (i + 1) * rows].astype(BF16)
        out_ref[:, i * count : (i + 1) * count] = part


def work(metric, amplitudes, virt_coef):
    rows, cols = amplitudes.shape
    half, width = rows // 2, metric.shape[1]
    by_core = pl.pallas_call(
        split_kernel,
        in_specs=[VMEM],
        out_specs=VMEM,
        out_shape=jax.ShapeDtypeStruct((8, 2, half, width), BF16),
        compiler_params=PARAMS,
    )(metric)
    ys = exchange(by_core.reshape(16, half, width), ("y", "c"))
    ys = ys.reshape(2, 1, 4, 2, half, width)
    wanted = jnp.broadcast_to(ys, (2, 2, 4, 2, half, width))
    part = exchange(wanted.reshape(4, 4, 2, half, width), ("xl", "xh"))
    part = part.reshape(2, 2, 4, 2, half, width)

    got = shifted(amplitudes, "c", 1)
    (packed,) = in_vmem(pack_kernel, [((rows, 2 * cols), BF16)], amplitudes, got)
    steps = [packed]
    for _ in range(1, 4):
        steps.append(ring_step(steps[-1]))
    swaps = [shifted(steps[s], "c", 1) for s in range(1, 4)]
    steps.append(ring_step(steps[3]))
    in_hbm = [pltpu.with_memory_space_constraint(a, pltpu.HBM) for a in swaps]
    shape = (half, 2 * cols)
    buffers = [pltpu.VMEM((3, rows, 2 * cols), BF16), pltpu.SemaphoreType.DMA((3,))]

    def on_blocks(kernel, outs, scratch, *args):
        spaces = [pltpu.HBM if a.dtype == F32 else pltpu.VMEM for a in args] + [pltpu.VMEM] * 5
        args = map(pltpu.with_memory_space_constraint, (*args, *steps), spaces)
        args = list(args)
        return pl.pallas_call(
            kernel,
            in_specs=[VMEM] * len(args) + [pl.BlockSpec(memory_space=pl.ANY)] * 3,
            out_specs=[VMEM] * len(outs),
            out_shape=[space(shape, dtype) for space, shape, dtype in outs],
            scratch_shapes=scratch + buffers,
            compiler_params=PARAMS,
        )(*args, *in_hbm)

    own, other, own_sent, other_sent = on_blocks(
        fitted_kernel,
        [(pltpu.VMEM, shape, F32), (pltpu.HBM, shape, F32)] + [(pltpu.VMEM, shape, BF16)] * 2,
        [],
        part,
    )
    own_arrived = shifted(other_sent, "xl", 1)
    other_arrived = shifted(own_sent, "xl", 1)
    (fitted,) = in_vmem(join_kernel, [(shape, BF16)], own, own_arrived)
    piece = (4, 2, half, half)
    slots = on_blocks(
        density_kernel,
        [(pltpu.VMEM, piece, BF16)] * 4,
        [pltpu.VMEM((4, *piece), BF16)],
        fitted, other, other_arrived,
    )
    arrived = [shifted_x(slots[s], s) for s in (2, 3, 1)]
    (xs,) = in_vmem(half_sum_kernel, [((8, 2, half, half), BF16)], slots[0], *arrived)
    got = exchange(xs.reshape(16, half, half), ("y", "c"))
    density = pl.pallas_call(
        last_sum_kernel,
        in_specs=[VMEM],
        out_specs=VMEM,
        out_shape=jax.ShapeDtypeStruct((rows // 16, 2, 8, half), F32),
        compiler_params=PARAMS,
    )(got.reshape(8, 2, half, half))

    got = exchange(fitted.reshape(16, 8, 2 * cols), ("y", "xh"))
    ao_count = virt_coef.shape[1]
    ao = pl.pallas_call(
        ao_kernel,
        in_specs=[VMEM] * 2,
        out_specs=VMEM,
        out_shape=jax.ShapeDtypeStruct((8, 16 * ao_count), BF16),
        compiler_params=PARAMS,
    )(got, pltpu.with_memory_space_constraint(virt_coef, pltpu.HBM))
    return density.reshape(rows, half), ao


def solution(mesh):
    split = Mesh(mesh.devices.reshape(2, 8, 8, 2, 2), ALL)
    return jax.shard_map(
        work,
        mesh=split,
        in_specs=(P(AUX, PAIR), P(AUX, PAIR), P()),
        out_specs=(P(AUX, PAIR), P(ALL, None)),
        check_vma=False,
    )
```

```python
import jax
import jax.numpy as jnp
from jax import lax
from jax.experimental import pallas as pl
from jax.experimental.pallas import tpu as pltpu
from jax.sharding import Mesh
from jax.sharding import PartitionSpec as P


AUX = ("xl", "z")
PAIR = ("y", "xh", "c")
ALL = AUX + PAIR
VMEM = pl.BlockSpec(memory_space=pltpu.VMEM)
PARAMS = pltpu.CompilerParams(vmem_limit_bytes=24 * 1024 * 1024)
F32, BF16 = jnp.float32, jnp.bfloat16


def in_vmem(kernel, outs, *args):
    args = [pltpu.with_memory_space_constraint(a, pltpu.VMEM) for a in args]
    return pl.pallas_call(
        kernel,
        in_specs=[VMEM] * len(args),
        out_specs=[VMEM] * len(outs),
        out_shape=[pltpu.VMEM(shape, dtype) for shape, dtype in outs],
        compiler_params=PARAMS,
    )(*args)


def shifted(x, axis, by):
    n = lax.axis_size(axis)
    return lax.ppermute(x, axis, [(i, (i + by) % n) for i in range(n)])


def exchange(x, axes):
    return lax.all_to_all(x, axes, split_axis=0, concat_axis=0, tiled=True)


def ring_step(x):
    n = lax.axis_size("z")
    moves = [(2 * i, 2 * ((i + 1) % n)) for i in range(n)]
    moves += [(2 * i + 1, 2 * ((i - 1) % n) + 1) for i in range(n)]
    return lax.ppermute(x, ("z", "c"), moves)


def shifted_x(x, by):
    at = lambda i: (i % 2) * 2 + i // 2
    return lax.ppermute(x, ("xl", "xh"), [(at(i), at((i + by) % 4)) for i in range(4)])


def blocks_of(refs):
    toward = 2 * lax.axis_index("c") - 1
    near = [(toward * s, ref[...]) for s, ref in enumerate(refs[:5])]
    return near + [(-toward * (i + 1), ref[...]) for i, ref in enumerate(refs[5:])]


def place(offset):
    at = lax.rem(lax.axis_index("z") + offset + 8, 8)
    return lax.rem(at, 2), lax.div(at, 2)


def pack_kernel(amp_ref, got_ref, out_ref):
    cols = got_ref.shape[1]
    first = lax.axis_index("c") == 0
    own, got = amp_ref[...], got_ref[...]
    out_ref[:, :cols] = jnp.where(first, own, got)
    out_ref[:, cols:] = jnp.where(first, got, own)


def split_kernel(in_ref, out_ref):
    n, cores, rows, cols = out_ref.shape
    groups = in_ref[...].astype(F32).reshape(rows // 8, cores, 8, cols)
    for c in range(cores):
        part = groups[:, c].reshape(rows, cols).astype(BF16)
        for i in range(n):
            out_ref[i, c] = part


def fitted_kernel(metric_ref, *refs):
    blocks = blocks_of(refs[:8])
    wide_refs, narrow_refs = refs[8:10], refs[10:12]
    xl = lax.axis_index("xl")
    rhs = jnp.concatenate([b for _, b in blocks], axis=0)
    for i, h in enumerate((xl, 1 - xl)):
        lhs = [metric_ref[(h, *place(o), j)] for o, _ in blocks for j in range(2)]
        out = jnp.dot(jnp.concatenate(lhs, axis=1), rhs, preferred_element_type=F32)
        wide_refs[i][...] = out
        narrow_refs[i][...] = out.astype(BF16)


def join_kernel(own_ref, arrived_ref, out_ref):
    out_ref[...] = (own_ref[...] + arrived_ref[...].astype(F32)).astype(BF16)


def density_kernel(own_ref, other_ref, arrived_ref, *refs):
    blocks, outs, all_ref = blocks_of(refs[:8]), refs[8:12], refs[12]
    xl = lax.axis_index("xl")
    x = 2 * lax.axis_index("xh") + xl
    other = (other_ref[...] + arrived_ref[...].astype(F32)).astype(BF16)
    fitted = jnp.concatenate([own_ref[...], other], axis=0)
    rows = own_ref.shape[0]
    for offset, block in blocks:
        out = lax.dot_general(
            block, fitted, (((1,), (1,)), ((), ())), preferred_element_type=F32
        ).astype(BF16)
        far, near = place(offset)
        half = out.shape[0] // 2
        for h, part in ((xl, out[:, :rows]), (1 - xl, out[:, rows:])):
            slot = lax.rem(2 * far + h + 4 - x, 4)
            for j in range(2):
                all_ref[slot, near, j] = part[j * half : (j + 1) * half]
    for s in range(4):
        outs[s][...] = all_ref[s]


def half_sum_kernel(here_ref, far_ref, left_ref, right_ref, out_ref):
    xl = lax.axis_index("xl")
    n = here_ref.shape[0]
    ours = here_ref[...].astype(F32) + far_ref[...].astype(F32)
    theirs = left_ref[...].astype(F32) + right_ref[...].astype(F32)
    out_ref[pl.ds(xl * n, n)] = ours.astype(BF16)
    out_ref[pl.ds((1 - xl) * n, n)] = theirs.astype(BF16)


def last_sum_kernel(in_ref, out_ref):
    groups, _, rows, _ = out_ref.shape
    for c in range(2):
        total = in_ref[0, c].astype(F32)
        for y in range(1, in_ref.shape[0]):
            total += in_ref[y, c].astype(F32)
        total = total.T
        for g in range(groups):
            out_ref[g, c] = total[g * rows : (g + 1) * rows]


def ao_kernel(got_ref, coef_ref, out_ref):
    n, rows, _ = got_ref.shape
    lhs = jnp.concatenate([got_ref[i].astype(F32) for i in range(n)], axis=0).astype(BF16)
    out = jnp.dot(lhs, coef_ref[...], preferred_element_type=F32)
    count = out.shape[1]
    for i in range(n):
        part = out[i * rows : (i + 1) * rows].astype(BF16)
        out_ref[:, i * count : (i + 1) * count] = part


def work(metric, amplitudes, virt_coef):
    rows, cols = amplitudes.shape
    half, width = rows // 2, metric.shape[1]
    by_core = pl.pallas_call(
        split_kernel,
        in_specs=[VMEM],
        out_specs=VMEM,
        out_shape=jax.ShapeDtypeStruct((8, 2, half, width), BF16),
        compiler_params=PARAMS,
    )(metric)
    ys = exchange(by_core.reshape(16, half, width), ("y", "c"))
    ys = ys.reshape(2, 1, 4, 2, half, width)
    wanted = jnp.broadcast_to(ys, (2, 2, 4, 2, half, width))
    part = exchange(wanted.reshape(4, 4, 2, half, width), ("xl", "xh"))
    part = part.reshape(2, 2, 4, 2, half, width)

    got = shifted(amplitudes, "c", 1)
    (packed,) = in_vmem(pack_kernel, [((rows, 2 * cols), BF16)], amplitudes, got)
    steps = [packed]
    for _ in range(1, 4):
        steps.append(ring_step(steps[-1]))
    swaps = [shifted(steps[s], "c", 1) for s in range(1, 4)]
    steps.append(ring_step(steps[3]))
    shape = (half, 2 * cols)

    def on_blocks(kernel, outs, scratch, *args):
        spaces = [pltpu.HBM if a.dtype == F32 else pltpu.VMEM for a in args] + [pltpu.VMEM] * 5 + [pltpu.HBM] * 3
        args = list(map(pltpu.with_memory_space_constraint, (*args, *steps, *swaps), spaces))
        return pl.pallas_call(
            kernel,
            in_specs=[VMEM] * len(args),
            out_specs=[VMEM] * len(outs),
            out_shape=[space(shape, dtype) for space, shape, dtype in outs],
            scratch_shapes=scratch,
            compiler_params=PARAMS,
        )(*args)

    own, other, own_sent, other_sent = on_blocks(
        fitted_kernel,
        [(pltpu.VMEM, shape, F32), (pltpu.HBM, shape, F32)] + [(pltpu.VMEM, shape, BF16)] * 2,
        [],
        part,
    )
    own_arrived = shifted(other_sent, "xl", 1)
    other_arrived = shifted(own_sent, "xl", 1)
    (fitted,) = in_vmem(join_kernel, [(shape, BF16)], own, own_arrived)
    piece = (4, 2, half, half)
    slots = on_blocks(
        density_kernel,
        [(pltpu.VMEM, piece, BF16)] * 4,
        [pltpu.VMEM((4, *piece), BF16)],
        fitted, other, other_arrived,
    )
    arrived = [shifted_x(slots[s], s) for s in (2, 3, 1)]
    (xs,) = in_vmem(half_sum_kernel, [((8, 2, half, half), BF16)], slots[0], *arrived)
    got = exchange(xs.reshape(16, half, half), ("y", "c"))
    density = pl.pallas_call(
        last_sum_kernel,
        in_specs=[VMEM],
        out_specs=VMEM,
        out_shape=jax.ShapeDtypeStruct((rows // 16, 2, 8, half), F32),
        compiler_params=PARAMS,
    )(got.reshape(8, 2, half, half))

    got = exchange(fitted.reshape(16, 8, 2 * cols), ("y", "xh"))
    ao_count = virt_coef.shape[1]
    ao = pl.pallas_call(
        ao_kernel,
        in_specs=[VMEM] * 2,
        out_specs=VMEM,
        out_shape=jax.ShapeDtypeStruct((8, 16 * ao_count), BF16),
        compiler_params=PARAMS,
    )(got, pltpu.with_memory_space_constraint(virt_coef, pltpu.HBM))
    return density.reshape(rows, half), ao


def solution(mesh):
    split = Mesh(mesh.devices.reshape(2, 8, 8, 2, 2), ALL)
    return jax.shard_map(
        work,
        mesh=split,
        in_specs=(P(AUX, PAIR), P(AUX, PAIR), P()),
        out_specs=(P(AUX, PAIR), P(ALL, None)),
        check_vma=False,
    )
```

```python
import jax
import jax.numpy as jnp
from jax import lax
from jax.experimental import pallas as pl
from jax.experimental.pallas import tpu as pltpu
from jax.sharding import Mesh
from jax.sharding import PartitionSpec as P


AUX = ("xl", "z")
PAIR = ("y", "xh", "c")
ALL = AUX + PAIR
VMEM = pl.BlockSpec(memory_space=pltpu.VMEM)
PARAMS = pltpu.CompilerParams(vmem_limit_bytes=24 * 1024 * 1024)
F32, BF16 = jnp.float32, jnp.bfloat16


def in_vmem(kernel, outs, *args):
    args = [pltpu.with_memory_space_constraint(a, pltpu.VMEM) for a in args]
    return pl.pallas_call(
        kernel,
        in_specs=[VMEM] * len(args),
        out_specs=[VMEM] * len(outs),
        out_shape=[pltpu.VMEM(shape, dtype) for shape, dtype in outs],
        compiler_params=PARAMS,
    )(*args)


def shifted(x, axis, by):
    n = lax.axis_size(axis)
    return lax.ppermute(x, axis, [(i, (i + by) % n) for i in range(n)])


def exchange(x, axes):
    return lax.all_to_all(x, axes, split_axis=0, concat_axis=0, tiled=True)


def ring_step(x):
    n = lax.axis_size("z")
    moves = [(2 * i, 2 * ((i + 1) % n)) for i in range(n)]
    moves += [(2 * i + 1, 2 * ((i - 1) % n) + 1) for i in range(n)]
    return lax.ppermute(x, ("z", "c"), moves)


def shifted_x(x, by):
    at = lambda i: (i % 2) * 2 + i // 2
    return lax.ppermute(x, ("xl", "xh"), [(at(i), at((i + by) % 4)) for i in range(4)])


def blocks_of(refs):
    toward = 2 * lax.axis_index("c") - 1
    near = [(toward * s, ref[...]) for s, ref in enumerate(refs[:5])]
    return near + [(-toward * (i + 1), ref[...]) for i, ref in enumerate(refs[5:])]


def place(offset):
    at = lax.rem(lax.axis_index("z") + offset + 8, 8)
    return lax.rem(at, 2), lax.div(at, 2)


def twice_kernel(in_ref, out_ref):
    for h in range(2):
        for i in range(2):
            out_ref[h, i] = in_ref[h]


def pack_kernel(amp_ref, got_ref, out_ref):
    cols = got_ref.shape[1]
    first = lax.axis_index("c") == 0
    own, got = amp_ref[...], got_ref[...]
    out_ref[:, :cols] = jnp.where(first, own, got)
    out_ref[:, cols:] = jnp.where(first, got, own)


def split_kernel(in_ref, out_ref):
    n, cores, rows, cols = out_ref.shape
    groups = in_ref[...].astype(F32).reshape(rows // 8, cores, 8, cols)
    for c in range(cores):
        part = groups[:, c].reshape(rows, cols).astype(BF16)
        for i in range(n):
            out_ref[i, c] = part


def fitted_kernel(metric_ref, *refs):
    blocks = blocks_of(refs[:8])
    wide_refs, narrow_refs = refs[8:10], refs[10:12]
    xl = lax.axis_index("xl")
    rhs = jnp.concatenate([b for _, b in blocks], axis=0)
    for i, h in enumerate((xl, 1 - xl)):
        lhs = [metric_ref[(h, *place(o), j)] for o, _ in blocks for j in range(2)]
        out = jnp.dot(jnp.concatenate(lhs, axis=1), rhs, preferred_element_type=F32)
        wide_refs[i][...] = out
        narrow_refs[i][...] = out.astype(BF16)


def join_kernel(own_ref, arrived_ref, out_ref):
    out_ref[...] = (own_ref[...] + arrived_ref[...].astype(F32)).astype(BF16)


def density_kernel(own_ref, other_ref, arrived_ref, *refs):
    blocks, outs, all_ref = blocks_of(refs[:8]), refs[8:12], refs[12]
    xl = lax.axis_index("xl")
    x = 2 * lax.axis_index("xh") + xl
    other = (other_ref[...] + arrived_ref[...].astype(F32)).astype(BF16)
    fitted = jnp.concatenate([own_ref[...], other], axis=0)
    rows = own_ref.shape[0]
    for offset, block in blocks:
        out = lax.dot_general(
            block, fitted, (((1,), (1,)), ((), ())), preferred_element_type=F32
        ).astype(BF16)
        far, near = place(offset)
        half = out.shape[0] // 2
        for h, part in ((xl, out[:, :rows]), (1 - xl, out[:, rows:])):
            slot = lax.rem(2 * far + h + 4 - x, 4)
            for j in range(2):
                all_ref[slot, near, j] = part[j * half : (j + 1) * half]
    for s in range(4):
        outs[s][...] = all_ref[s]


def half_sum_kernel(here_ref, far_ref, left_ref, right_ref, out_ref):
    xl = lax.axis_index("xl")
    n = here_ref.shape[0]
    ours = here_ref[...].astype(F32) + far_ref[...].astype(F32)
    theirs = left_ref[...].astype(F32) + right_ref[...].astype(F32)
    out_ref[pl.ds(xl * n, n)] = ours.astype(BF16)
    out_ref[pl.ds((1 - xl) * n, n)] = theirs.astype(BF16)


def last_sum_kernel(in_ref, out_ref):
    groups, _, rows, _ = out_ref.shape
    for c in range(2):
        total = in_ref[0, c].astype(F32)
        for y in range(1, in_ref.shape[0]):
            total += in_ref[y, c].astype(F32)
        total = total.T
        for g in range(groups):
            out_ref[g, c] = total[g * rows : (g + 1) * rows]


def ao_kernel(got_ref, coef_ref, out_ref):
    n, rows, _ = got_ref.shape
    lhs = jnp.concatenate([got_ref[i].astype(F32) for i in range(n)], axis=0).astype(BF16)
    out = jnp.dot(lhs, coef_ref[...], preferred_element_type=F32)
    count = out.shape[1]
    for i in range(n):
        part = out[i * rows : (i + 1) * rows].astype(BF16)
        out_ref[:, i * count : (i + 1) * count] = part


def work(metric, amplitudes, virt_coef):
    rows, cols = amplitudes.shape
    half, width = rows // 2, metric.shape[1]
    by_core = pl.pallas_call(
        split_kernel,
        in_specs=[VMEM],
        out_specs=VMEM,
        out_shape=jax.ShapeDtypeStruct((8, 2, half, width), BF16),
        compiler_params=PARAMS,
    )(pltpu.with_memory_space_constraint(metric, pltpu.HBM))
    ys = exchange(by_core.reshape(16, half, width), ("y", "c"))
    wanted = pl.pallas_call(
        twice_kernel,
        in_specs=[VMEM],
        out_specs=VMEM,
        out_shape=jax.ShapeDtypeStruct((2, 2, 4, 2, half, width), BF16),
        compiler_params=PARAMS,
    )(ys.reshape(2, 4, 2, half, width))
    part = exchange(wanted.reshape(4, 4, 2, half, width), ("xl", "xh"))
    part = part.reshape(2, 2, 4, 2, half, width)

    got = shifted(amplitudes, "c", 1)
    packed = pl.pallas_call(
        pack_kernel,
        in_specs=[VMEM] * 2,
        out_specs=VMEM,
        out_shape=pltpu.VMEM((rows, 2 * cols), BF16),
        compiler_params=PARAMS,
    )(
        pltpu.with_memory_space_constraint(amplitudes, pltpu.HBM),
        pltpu.with_memory_space_constraint(got, pltpu.VMEM),
    )
    steps = [packed]
    for _ in range(1, 4):
        steps.append(ring_step(steps[-1]))
    swaps = [shifted(steps[s], "c", 1) for s in range(1, 4)]
    steps.append(ring_step(steps[3]))
    shape = (half, 2 * cols)

    def on_blocks(kernel, outs, scratch, *args):
        spaces = [pltpu.HBM if a.dtype == F32 else pltpu.VMEM for a in args] + [pltpu.VMEM] * 5 + [pltpu.HBM] * 3
        args = list(map(pltpu.with_memory_space_constraint, (*args, *steps, *swaps), spaces))
        return pl.pallas_call(
            kernel,
            in_specs=[VMEM] * len(args),
            out_specs=[VMEM] * len(outs),
            out_shape=[space(shape, dtype) for space, shape, dtype in outs],
            scratch_shapes=scratch,
            compiler_params=PARAMS,
        )(*args)

    own, other, own_sent, other_sent = on_blocks(
        fitted_kernel,
        [(pltpu.VMEM, shape, F32), (pltpu.HBM, shape, F32)] + [(pltpu.VMEM, shape, BF16)] * 2,
        [],
        part,
    )
    own_arrived = shifted(other_sent, "xl", 1)
    other_arrived = shifted(own_sent, "xl", 1)
    (fitted,) = in_vmem(join_kernel, [(shape, BF16)], own, own_arrived)
    piece = (4, 2, half, half)
    slots = on_blocks(
        density_kernel,
        [(pltpu.VMEM, piece, BF16)] * 4,
        [pltpu.VMEM((4, *piece), BF16)],
        fitted, other, other_arrived,
    )
    arrived = [shifted_x(slots[s], s) for s in (2, 3, 1)]
    (xs,) = in_vmem(half_sum_kernel, [((8, 2, half, half), BF16)], slots[0], *arrived)
    got = exchange(xs.reshape(16, half, half), ("y", "c"))
    density = pl.pallas_call(
        last_sum_kernel,
        in_specs=[VMEM],
        out_specs=VMEM,
        out_shape=jax.ShapeDtypeStruct((rows // 16, 2, 8, half), F32),
        compiler_params=PARAMS,
    )(got.reshape(8, 2, half, half))

    got = exchange(fitted.reshape(16, 8, 2 * cols), ("y", "xh"))
    ao_count = virt_coef.shape[1]
    ao = pl.pallas_call(
        ao_kernel,
        in_specs=[VMEM] * 2,
        out_specs=VMEM,
        out_shape=jax.ShapeDtypeStruct((8, 16 * ao_count), BF16),
        compiler_params=PARAMS,
    )(got, pltpu.with_memory_space_constraint(virt_coef, pltpu.HBM))
    return density.reshape(rows, half), ao


def solution(mesh):
    split = Mesh(mesh.devices.reshape(2, 8, 8, 2, 2), ALL)
    return jax.shard_map(
        work,
        mesh=split,
        in_specs=(P(AUX, PAIR), P(AUX, PAIR), P()),
        out_specs=(P(AUX, PAIR), P(ALL, None)),
        check_vma=False,
    )
```

```python
import jax
import jax.numpy as jnp
from jax import lax
from jax.experimental import pallas as pl
from jax.experimental.pallas import tpu as pltpu
from jax.sharding import Mesh
from jax.sharding import PartitionSpec as P


AUX = ("xl", "z")
PAIR = ("y", "xh", "c")
ALL = AUX + PAIR
VMEM = pl.BlockSpec(memory_space=pltpu.VMEM)
PARAMS = pltpu.CompilerParams(vmem_limit_bytes=24 * 1024 * 1024)
F32, BF16 = jnp.float32, jnp.bfloat16


def in_vmem(kernel, outs, *args):
    args = [pltpu.with_memory_space_constraint(a, pltpu.VMEM) for a in args]
    return pl.pallas_call(
        kernel,
        in_specs=[VMEM] * len(args),
        out_specs=[VMEM] * len(outs),
        out_shape=[pltpu.VMEM(shape, dtype) for shape, dtype in outs],
        compiler_params=PARAMS,
    )(*args)


def shifted(x, axis, by):
    n = lax.axis_size(axis)
    return lax.ppermute(x, axis, [(i, (i + by) % n) for i in range(n)])


def exchange(x, axes):
    return lax.all_to_all(x, axes, split_axis=0, concat_axis=0, tiled=True)


def ring_step(x):
    n = lax.axis_size("z")
    moves = [(2 * i, 2 * ((i + 1) % n)) for i in range(n)]
    moves += [(2 * i + 1, 2 * ((i - 1) % n) + 1) for i in range(n)]
    return lax.ppermute(x, ("z", "c"), moves)


def shifted_x(x, by):
    at = lambda i: (i % 2) * 2 + i // 2
    return lax.ppermute(x, ("xl", "xh"), [(at(i), at((i + by) % 4)) for i in range(4)])


NEAR = 4


def toward(s):
    return (2 * lax.axis_index("c") - 1) * s


FAR_STEPS = (4, -1, -2, -3)


def copies_of(refs, bufs, sems):
    copies = [pltpu.make_async_copy(ref, bufs.at[i], sems.at[i]) for i, ref in enumerate(refs)]
    for copy in copies:
        copy.start()
    return copies


def place(offset):
    at = lax.rem(lax.axis_index("z") + offset + 8, 8)
    return lax.rem(at, 2), lax.div(at, 2)


def twice_kernel(in_ref, out_ref):
    for h in range(2):
        for i in range(2):
            out_ref[h, i] = in_ref[h]


def pack_kernel(amp_ref, got_ref, out_ref):
    cols = got_ref.shape[1]
    first = lax.axis_index("c") == 0
    own, got = amp_ref[...], got_ref[...]
    out_ref[:, :cols] = jnp.where(first, own, got)
    out_ref[:, cols:] = jnp.where(first, got, own)


def split_kernel(in_ref, out_ref):
    n, cores, rows, cols = out_ref.shape
    groups = in_ref[...].astype(F32).reshape(rows // 8, cores, 8, cols)
    for c in range(cores):
        part = groups[:, c].reshape(rows, cols).astype(BF16)
        for i in range(n):
            out_ref[i, c] = part


def fitted_kernel(metric_ref, *refs):
    near_refs, far_refs = refs[:NEAR], refs[NEAR : 2 * NEAR]
    wide_refs, narrow_refs, (bufs, sems) = refs[8:10], refs[10:12], refs[12:]
    copies = copies_of(far_refs, bufs, sems)
    xl = lax.axis_index("xl")

    def product(h, steps, blocks):
        lhs = [metric_ref[(h, *place(toward(s)), j)] for s in steps for j in range(2)]
        rhs = jnp.concatenate(blocks, axis=0)
        return jnp.dot(jnp.concatenate(lhs, axis=1), rhs, preferred_element_type=F32)

    halves = (xl, 1 - xl)
    for i, h in enumerate(halves):
        wide_refs[i][...] = product(h, range(NEAR), [ref[...] for ref in near_refs])
    for copy in copies:
        copy.wait()
    for i, h in enumerate(halves):
        out = wide_refs[i][...] + product(h, FAR_STEPS, [bufs[k] for k in range(NEAR)])
        wide_refs[i][...] = out
        narrow_refs[i][...] = out.astype(BF16)


def join_kernel(own_ref, arrived_ref, out_ref):
    out_ref[...] = (own_ref[...] + arrived_ref[...].astype(F32)).astype(BF16)


def density_kernel(own_ref, arrived_ref, *refs):
    near_refs, far_refs, other_ref = refs[:NEAR], refs[NEAR : 2 * NEAR], refs[8]
    outs, (all_ref, bufs, sems, other_buf, other_sem) = refs[9:13], refs[13:]
    other_copy = pltpu.make_async_copy(other_ref, other_buf, other_sem)
    other_copy.start()
    copies = copies_of(far_refs, bufs, sems)
    xl = lax.axis_index("xl")
    x = 2 * lax.axis_index("xh") + xl
    rows = own_ref.shape[0]

    def put(step, block, fitted, halves):
        out = lax.dot_general(
            block, fitted, (((1,), (1,)), ((), ())), preferred_element_type=F32
        ).astype(BF16)
        far, near = place(toward(step))
        half = out.shape[0] // 2
        for i, h in enumerate(halves):
            slot = lax.rem(2 * far + h + 4 - x, 4)
            for j in range(2):
                part = out[j * half : (j + 1) * half, i * rows : (i + 1) * rows]
                all_ref[slot, near, j] = part

    own = own_ref[...]
    for s, ref in enumerate(near_refs):
        put(s, ref[...], own, (xl,))
    other_copy.wait()
    other = (other_buf[...] + arrived_ref[...].astype(F32)).astype(BF16)
    for s, ref in enumerate(near_refs):
        put(s, ref[...], other, (1 - xl,))
    for copy in copies:
        copy.wait()
    both = jnp.concatenate([own, other], axis=0)
    for i, s in enumerate(FAR_STEPS):
        put(s, bufs[i], both, (xl, 1 - xl))
    for s in range(4):
        outs[s][...] = all_ref[s]


def half_sum_kernel(here_ref, far_ref, left_ref, right_ref, out_ref):
    xl = lax.axis_index("xl")
    n = here_ref.shape[0]
    ours = here_ref[...].astype(F32) + far_ref[...].astype(F32)
    theirs = left_ref[...].astype(F32) + right_ref[...].astype(F32)
    out_ref[pl.ds(xl * n, n)] = ours.astype(BF16)
    out_ref[pl.ds((1 - xl) * n, n)] = theirs.astype(BF16)


def last_sum_kernel(in_ref, out_ref):
    groups, _, rows, _ = out_ref.shape
    for c in range(2):
        total = in_ref[0, c].astype(F32)
        for y in range(1, in_ref.shape[0]):
            total += in_ref[y, c].astype(F32)
        total = total.T
        for g in range(groups):
            out_ref[g, c] = total[g * rows : (g + 1) * rows]


def ao_kernel(got_ref, coef_ref, out_ref):
    n, rows, _ = got_ref.shape
    lhs = jnp.concatenate([got_ref[i].astype(F32) for i in range(n)], axis=0).astype(BF16)
    out = jnp.dot(lhs, coef_ref[...], preferred_element_type=F32)
    count = out.shape[1]
    for i in range(n):
        part = out[i * rows : (i + 1) * rows].astype(BF16)
        out_ref[:, i * count : (i + 1) * count] = part


def work(metric, amplitudes, virt_coef):
    rows, cols = amplitudes.shape
    half, width = rows // 2, metric.shape[1]
    by_core = pl.pallas_call(
        split_kernel,
        in_specs=[VMEM],
        out_specs=VMEM,
        out_shape=jax.ShapeDtypeStruct((8, 2, half, width), BF16),
        compiler_params=PARAMS,
    )(pltpu.with_memory_space_constraint(metric, pltpu.HBM))
    ys = exchange(by_core.reshape(16, half, width), ("y", "c"))
    wanted = pl.pallas_call(
        twice_kernel,
        in_specs=[VMEM],
        out_specs=VMEM,
        out_shape=jax.ShapeDtypeStruct((2, 2, 4, 2, half, width), BF16),
        compiler_params=PARAMS,
    )(ys.reshape(2, 4, 2, half, width))
    part = exchange(wanted.reshape(4, 4, 2, half, width), ("xl", "xh"))
    part = part.reshape(2, 2, 4, 2, half, width)

    got = shifted(amplitudes, "c", 1)
    packed = pl.pallas_call(
        pack_kernel,
        in_specs=[VMEM] * 2,
        out_specs=VMEM,
        out_shape=pltpu.VMEM((rows, 2 * cols), BF16),
        compiler_params=PARAMS,
    )(
        pltpu.with_memory_space_constraint(amplitudes, pltpu.HBM),
        pltpu.with_memory_space_constraint(got, pltpu.VMEM),
    )
    steps = [packed]
    for _ in range(1, 4):
        steps.append(ring_step(steps[-1]))
    swaps = [shifted(steps[s], "c", 1) for s in range(1, 4)]
    steps.append(ring_step(steps[3]))
    shape = (half, 2 * cols)

    near, far = steps[:NEAR], [steps[NEAR], *swaps]

    def on_blocks(kernel, outs, scratch, args, last=()):
        in_near = [pltpu.with_memory_space_constraint(a, pltpu.VMEM) for a in (*args, *near)]
        in_far = [pltpu.with_memory_space_constraint(a, pltpu.HBM) for a in (*far, *last)]
        buffers = [pltpu.VMEM((NEAR, rows, 2 * cols), BF16), pltpu.SemaphoreType.DMA((NEAR,))]
        return pl.pallas_call(
            kernel,
            in_specs=[VMEM] * len(in_near) + [pl.BlockSpec(memory_space=pl.ANY)] * len(in_far),
            out_specs=[VMEM] * len(outs),
            out_shape=[space(shape, dtype) for space, shape, dtype in outs],
            scratch_shapes=scratch[:1] + buffers + scratch[1:],
            compiler_params=PARAMS,
        )(*in_near, *in_far)

    own, other, own_sent, other_sent = on_blocks(
        fitted_kernel,
        [(pltpu.VMEM, shape, F32), (pltpu.HBM, shape, F32)] + [(pltpu.VMEM, shape, BF16)] * 2,
        [],
        [part],
    )
    own_arrived = shifted(other_sent, "xl", 1)
    other_arrived = shifted(own_sent, "xl", 1)
    (fitted,) = in_vmem(join_kernel, [(shape, BF16)], own, own_arrived)
    piece = (4, 2, half, half)
    slots = on_blocks(
        density_kernel,
        [(pltpu.VMEM, piece, BF16)] * 4,
        [pltpu.VMEM((4, *piece), BF16), pltpu.VMEM(shape, F32), pltpu.SemaphoreType.DMA],
        [fitted, other_arrived],
        [other],
    )
    arrived = [shifted_x(slots[s], s) for s in (2, 3, 1)]
    (xs,) = in_vmem(half_sum_kernel, [((8, 2, half, half), BF16)], slots[0], *arrived)
    got = exchange(xs.reshape(16, half, half), ("y", "c"))
    density = pl.pallas_call(
        last_sum_kernel,
        in_specs=[VMEM],
        out_specs=VMEM,
        out_shape=jax.ShapeDtypeStruct((rows // 16, 2, 8, half), F32),
        compiler_params=PARAMS,
    )(got.reshape(8, 2, half, half))

    got = exchange(fitted.reshape(16, 8, 2 * cols), ("y", "xh"))
    ao_count = virt_coef.shape[1]
    ao = pl.pallas_call(
        ao_kernel,
        in_specs=[VMEM] * 2,
        out_specs=VMEM,
        out_shape=jax.ShapeDtypeStruct((8, 16 * ao_count), BF16),
        compiler_params=PARAMS,
    )(got, pltpu.with_memory_space_constraint(virt_coef, pltpu.HBM))
    return density.reshape(rows, half), ao


def solution(mesh):
    split = Mesh(mesh.devices.reshape(2, 8, 8, 2, 2), ALL)
    return jax.shard_map(
        work,
        mesh=split,
        in_specs=(P(AUX, PAIR), P(AUX, PAIR), P()),
        out_specs=(P(AUX, PAIR), P(ALL, None)),
        check_vma=False,
    )
```

```python
import jax
import jax.numpy as jnp
from jax import lax
from jax.experimental import pallas as pl
from jax.experimental.pallas import tpu as pltpu
from jax.sharding import Mesh
from jax.sharding import PartitionSpec as P


AUX = ("xl", "z")
PAIR = ("y", "xh", "c")
ALL = AUX + PAIR
VMEM = pl.BlockSpec(memory_space=pltpu.VMEM)
PARAMS = pltpu.CompilerParams(vmem_limit_bytes=24 * 1024 * 1024)
F32, BF16 = jnp.float32, jnp.bfloat16


def in_vmem(kernel, outs, *args):
    args = [pltpu.with_memory_space_constraint(a, pltpu.VMEM) for a in args]
    return pl.pallas_call(
        kernel,
        in_specs=[VMEM] * len(args),
        out_specs=[VMEM] * len(outs),
        out_shape=[pltpu.VMEM(shape, dtype) for shape, dtype in outs],
        compiler_params=PARAMS,
    )(*args)


def shifted(x, axis, by):
    n = lax.axis_size(axis)
    return lax.ppermute(x, axis, [(i, (i + by) % n) for i in range(n)])


def exchange(x, axes):
    return lax.all_to_all(x, axes, split_axis=0, concat_axis=0, tiled=True)


def ring_step(x):
    n = lax.axis_size("z")
    moves = [(2 * i, 2 * ((i + 1) % n)) for i in range(n)]
    moves += [(2 * i + 1, 2 * ((i - 1) % n) + 1) for i in range(n)]
    return lax.ppermute(x, ("z", "c"), moves)


def shifted_x(x, by):
    at = lambda i: (i % 2) * 2 + i // 2
    return lax.ppermute(x, ("xl", "xh"), [(at(i), at((i + by) % 4)) for i in range(4)])


def blocks_of(refs):
    toward = 2 * lax.axis_index("c") - 1
    near = [(toward * s, ref[...]) for s, ref in enumerate(refs[:5])]
    return near + [(-toward * (i + 1), ref[...]) for i, ref in enumerate(refs[5:])]


def place(offset):
    at = lax.rem(lax.axis_index("z") + offset + 8, 8)
    return lax.rem(at, 2), lax.div(at, 2)


def twice_kernel(in_ref, out_ref):
    for h in range(2):
        for i in range(2):
            out_ref[h, i] = in_ref[h]


def pack_kernel(amp_ref, got_ref, out_ref):
    cols = got_ref.shape[1]
    first = lax.axis_index("c") == 0
    own, got = amp_ref[...], got_ref[...]
    out_ref[:, :cols] = jnp.where(first, own, got)
    out_ref[:, cols:] = jnp.where(first, got, own)


def split_kernel(in_ref, out_ref):
    n, cores, rows, cols = out_ref.shape
    groups = in_ref[...].astype(F32).reshape(rows // 8, cores, 8, cols)
    for c in range(cores):
        part = groups[:, c].reshape(rows, cols).astype(BF16)
        for i in range(n):
            out_ref[i, c] = part


def fitted_kernel(metric_ref, *refs):
    blocks = blocks_of(refs[:8])
    wide_refs, narrow_refs = refs[8:10], refs[10:12]
    xl = lax.axis_index("xl")
    rhs = jnp.concatenate([b for _, b in blocks], axis=0)
    lhs = [
        jnp.concatenate([metric_ref[(h, *place(o), j)] for o, _ in blocks for j in range(2)], axis=1)
        for h in (xl, 1 - xl)
    ]
    out = jnp.dot(jnp.concatenate(lhs, axis=0), rhs, preferred_element_type=F32)
    rows = out.shape[0] // 2
    for i in range(2):
        part = out[i * rows : (i + 1) * rows]
        wide_refs[i][...] = part
        narrow_refs[i][...] = part.astype(BF16)


def join_kernel(own_ref, arrived_ref, out_ref):
    out_ref[...] = (own_ref[...] + arrived_ref[...].astype(F32)).astype(BF16)


def density_kernel(own_ref, other_ref, arrived_ref, *refs):
    blocks, outs, all_ref = blocks_of(refs[:8]), refs[8:12], refs[12]
    xl = lax.axis_index("xl")
    x = 2 * lax.axis_index("xh") + xl
    other = (other_ref[...] + arrived_ref[...].astype(F32)).astype(BF16)
    fitted = jnp.concatenate([own_ref[...], other], axis=0)
    rows = own_ref.shape[0]
    amp = jnp.concatenate([b for _, b in blocks], axis=0)
    whole = lax.dot_general(amp, fitted, (((1,), (1,)), ((), ())), preferred_element_type=F32)
    height = blocks[0][1].shape[0]
    half = height // 2
    for i, (offset, _) in enumerate(blocks):
        out = whole[i * height : (i + 1) * height].astype(BF16)
        far, near = place(offset)
        for h, part in ((xl, out[:, :rows]), (1 - xl, out[:, rows:])):
            slot = lax.rem(2 * far + h + 4 - x, 4)
            for j in range(2):
                all_ref[slot, near, j] = part[j * half : (j + 1) * half]
    for s in range(4):
        outs[s][...] = all_ref[s]


def half_sum_kernel(here_ref, far_ref, left_ref, right_ref, out_ref):
    xl = lax.axis_index("xl")
    n = here_ref.shape[0]
    ours = here_ref[...].astype(F32) + far_ref[...].astype(F32)
    theirs = left_ref[...].astype(F32) + right_ref[...].astype(F32)
    out_ref[pl.ds(xl * n, n)] = ours.astype(BF16)
    out_ref[pl.ds((1 - xl) * n, n)] = theirs.astype(BF16)


def last_sum_kernel(in_ref, out_ref):
    groups, _, rows, _ = out_ref.shape
    for c in range(2):
        total = in_ref[0, c].astype(F32)
        for y in range(1, in_ref.shape[0]):
            total += in_ref[y, c].astype(F32)
        total = total.T
        for g in range(groups):
            out_ref[g, c] = total[g * rows : (g + 1) * rows]


def ao_kernel(got_ref, coef_ref, out_ref):
    n, rows, _ = got_ref.shape
    lhs = jnp.concatenate([got_ref[i].astype(F32) for i in range(n)], axis=0).astype(BF16)
    out = jnp.dot(lhs, coef_ref[...], preferred_element_type=F32)
    count = out.shape[1]
    for i in range(n):
        part = out[i * rows : (i + 1) * rows].astype(BF16)
        out_ref[:, i * count : (i + 1) * count] = part


def work(metric, amplitudes, virt_coef):
    rows, cols = amplitudes.shape
    half, width = rows // 2, metric.shape[1]
    by_core = pl.pallas_call(
        split_kernel,
        in_specs=[VMEM],
        out_specs=VMEM,
        out_shape=jax.ShapeDtypeStruct((8, 2, half, width), BF16),
        compiler_params=PARAMS,
    )(pltpu.with_memory_space_constraint(metric, pltpu.HBM))
    ys = exchange(by_core.reshape(16, half, width), ("y", "c"))
    wanted = pl.pallas_call(
        twice_kernel,
        in_specs=[VMEM],
        out_specs=VMEM,
        out_shape=jax.ShapeDtypeStruct((2, 2, 4, 2, half, width), BF16),
        compiler_params=PARAMS,
    )(ys.reshape(2, 4, 2, half, width))
    part = exchange(wanted.reshape(4, 4, 2, half, width), ("xl", "xh"))
    part = part.reshape(2, 2, 4, 2, half, width)

    got = shifted(amplitudes, "c", 1)
    packed = pl.pallas_call(
        pack_kernel,
        in_specs=[VMEM] * 2,
        out_specs=VMEM,
        out_shape=pltpu.VMEM((rows, 2 * cols), BF16),
        compiler_params=PARAMS,
    )(
        pltpu.with_memory_space_constraint(amplitudes, pltpu.HBM),
        pltpu.with_memory_space_constraint(got, pltpu.VMEM),
    )
    steps = [packed]
    for _ in range(1, 4):
        steps.append(ring_step(steps[-1]))
    swaps = [shifted(steps[s], "c", 1) for s in range(1, 4)]
    steps.append(ring_step(steps[3]))
    shape = (half, 2 * cols)

    def on_blocks(kernel, outs, scratch, *args):
        small = (a.dtype == BF16 and a.ndim == 2 for a in args)
        spaces = [pltpu.VMEM if fits else pltpu.HBM for fits in small]
        spaces += [pltpu.VMEM] * 4 + [pltpu.HBM] + [pltpu.VMEM] * 2 + [pltpu.HBM]
        args = list(map(pltpu.with_memory_space_constraint, (*args, *steps, *swaps), spaces))
        return pl.pallas_call(
            kernel,
            in_specs=[VMEM] * len(args),
            out_specs=[VMEM] * len(outs),
            out_shape=[space(shape, dtype) for space, shape, dtype in outs],
            scratch_shapes=scratch,
            compiler_params=PARAMS,
        )(*args)

    own, other, own_sent, other_sent = on_blocks(
        fitted_kernel,
        [(pltpu.VMEM, shape, F32), (pltpu.HBM, shape, F32)] + [(pltpu.VMEM, shape, BF16)] * 2,
        [],
        part,
    )
    own_arrived = shifted(other_sent, "xl", 1)
    other_arrived = shifted(own_sent, "xl", 1)
    (fitted,) = in_vmem(join_kernel, [(shape, BF16)], own, own_arrived)
    piece = (4, 2, half, half)
    slots = on_blocks(
        density_kernel,
        [(space, piece, BF16) for space in (pltpu.HBM, pltpu.VMEM) * 2],
        [pltpu.VMEM((4, *piece), BF16)],
        fitted, other, other_arrived,
    )
    arrived = [shifted_x(slots[s], s) for s in (2, 3, 1)]
    (xs,) = in_vmem(half_sum_kernel, [((8, 2, half, half), BF16)], slots[0], *arrived)
    got = exchange(xs.reshape(16, half, half), ("y", "c"))
    density = pl.pallas_call(
        last_sum_kernel,
        in_specs=[VMEM],
        out_specs=VMEM,
        out_shape=jax.ShapeDtypeStruct((rows // 16, 2, 8, half), F32),
        compiler_params=PARAMS,
    )(got.reshape(8, 2, half, half))

    got = exchange(fitted.reshape(16, 8, 2 * cols), ("y", "xh"))
    ao_count = virt_coef.shape[1]
    ao = pl.pallas_call(
        ao_kernel,
        in_specs=[VMEM] * 2,
        out_specs=VMEM,
        out_shape=jax.ShapeDtypeStruct((8, 16 * ao_count), BF16),
        compiler_params=PARAMS,
    )(got, pltpu.with_memory_space_constraint(virt_coef, pltpu.HBM))
    return density.reshape(rows, half), ao


def solution(mesh):
    split = Mesh(mesh.devices.reshape(2, 8, 8, 2, 2), ALL)
    return jax.shard_map(
        work,
        mesh=split,
        in_specs=(P(AUX, PAIR), P(AUX, PAIR), P()),
        out_specs=(P(AUX, PAIR), P(ALL, None)),
        check_vma=False,
    )
```

```python
import jax
import jax.numpy as jnp
from jax import lax
from jax.experimental import pallas as pl
from jax.experimental.pallas import tpu as pltpu
from jax.sharding import Mesh
from jax.sharding import PartitionSpec as P


AUX = ("xl", "z")
PAIR = ("y", "xh", "c")
ALL = AUX + PAIR
VMEM = pl.BlockSpec(memory_space=pltpu.VMEM)
PARAMS = pltpu.CompilerParams(vmem_limit_bytes=24 * 1024 * 1024)
F32, BF16 = jnp.float32, jnp.bfloat16


def in_vmem(kernel, outs, *args):
    args = [pltpu.with_memory_space_constraint(a, pltpu.VMEM) for a in args]
    return pl.pallas_call(
        kernel,
        in_specs=[VMEM] * len(args),
        out_specs=[VMEM] * len(outs),
        out_shape=[pltpu.VMEM(shape, dtype) for shape, dtype in outs],
        compiler_params=PARAMS,
    )(*args)


def shifted(x, axis, by):
    n = lax.axis_size(axis)
    return lax.ppermute(x, axis, [(i, (i + by) % n) for i in range(n)])


def exchange(x, axes):
    return lax.all_to_all(x, axes, split_axis=0, concat_axis=0, tiled=True)


def ring_step(x):
    n = lax.axis_size("z")
    moves = [(2 * i, 2 * ((i + 1) % n)) for i in range(n)]
    moves += [(2 * i + 1, 2 * ((i - 1) % n) + 1) for i in range(n)]
    return lax.ppermute(x, ("z", "c"), moves)


def shifted_x(x, by):
    at = lambda i: (i % 2) * 2 + i // 2
    return lax.ppermute(x, ("xl", "xh"), [(at(i), at((i + by) % 4)) for i in range(4)])


def blocks_of(refs):
    toward = 2 * lax.axis_index("c") - 1
    near = [(toward * s, ref[...]) for s, ref in enumerate(refs[:5])]
    return near + [(-toward * (i + 1), ref[...]) for i, ref in enumerate(refs[5:])]


def place(offset):
    at = lax.rem(lax.axis_index("z") + offset + 8, 8)
    return lax.rem(at, 2), lax.div(at, 2)


def twice_kernel(in_ref, out_ref):
    for h in range(2):
        for i in range(2):
            out_ref[h, i] = in_ref[h]


def pack_kernel(amp_ref, got_ref, out_ref):
    cols = got_ref.shape[1]
    first = lax.axis_index("c") == 0
    own, got = amp_ref[...], got_ref[...]
    out_ref[:, :cols] = jnp.where(first, own, got)
    out_ref[:, cols:] = jnp.where(first, got, own)


def split_kernel(in_ref, out_ref):
    n, cores, rows, cols = out_ref.shape
    groups = in_ref[...].astype(F32).reshape(rows // 8, cores, 8, cols)
    for c in range(cores):
        part = groups[:, c].reshape(rows, cols).astype(BF16)
        for i in range(n):
            out_ref[i, c] = part


def fitted_kernel(metric_ref, *refs):
    blocks = blocks_of(refs[:8])
    wide_refs, narrow_refs = refs[8:10], refs[10:12]
    xl = lax.axis_index("xl")
    rhs = jnp.concatenate([b for _, b in blocks], axis=0)
    lhs = [
        jnp.concatenate([metric_ref[(h, *place(o), j)] for o, _ in blocks for j in range(2)], axis=1)
        for h in (xl, 1 - xl)
    ]
    out = jnp.dot(jnp.concatenate(lhs, axis=0), rhs, preferred_element_type=F32)
    rows = out.shape[0] // 2
    for i in range(2):
        part = out[i * rows : (i + 1) * rows]
        wide_refs[i][...] = part
        narrow_refs[i][...] = part.astype(BF16)


def join_kernel(own_ref, arrived_ref, out_ref):
    out_ref[...] = (own_ref[...] + arrived_ref[...].astype(F32)).astype(BF16)


def density_kernel(own_ref, other_ref, arrived_ref, *refs):
    blocks, outs, all_ref = blocks_of(refs[:8]), refs[8:12], refs[12]
    xl = lax.axis_index("xl")
    x = 2 * lax.axis_index("xh") + xl
    other = (other_ref[...] + arrived_ref[...].astype(F32)).astype(BF16)
    fitted = jnp.concatenate([own_ref[...], other], axis=0)
    rows = own_ref.shape[0]
    amp = jnp.concatenate([b for _, b in blocks], axis=0)
    whole = lax.dot_general(amp, fitted, (((1,), (1,)), ((), ())), preferred_element_type=F32)
    height = blocks[0][1].shape[0]
    half = height // 2
    for i, (offset, _) in enumerate(blocks):
        out = whole[i * height : (i + 1) * height].astype(BF16)
        far, near = place(offset)
        for h, part in ((xl, out[:, :rows]), (1 - xl, out[:, rows:])):
            slot = lax.rem(2 * far + h + 4 - x, 4)
            for j in range(2):
                all_ref[slot, near, j] = part[j * half : (j + 1) * half]
    for s in range(4):
        outs[s][...] = all_ref[s]


def half_sum_kernel(here_ref, far_ref, left_ref, right_ref, out_ref):
    xl = lax.axis_index("xl")
    n = here_ref.shape[0]
    ours = here_ref[...].astype(F32) + far_ref[...].astype(F32)
    theirs = left_ref[...].astype(F32) + right_ref[...].astype(F32)
    out_ref[pl.ds(xl * n, n)] = ours.astype(BF16)
    out_ref[pl.ds((1 - xl) * n, n)] = theirs.astype(BF16)


def last_sum_kernel(in_ref, out_ref):
    groups, _, rows, _ = out_ref.shape
    for c in range(2):
        total = in_ref[0, c].astype(F32)
        for y in range(1, in_ref.shape[0]):
            total += in_ref[y, c].astype(F32)
        total = total.T
        for g in range(groups):
            out_ref[g, c] = total[g * rows : (g + 1) * rows]


def pick_kernel(got_ref, keep_ref, send_ref):
    xh = lax.axis_index("xh")
    for y in range(got_ref.shape[0]):
        keep_ref[y] = got_ref[y, xh]
        send_ref[y] = got_ref[y, 1 - xh]


def ao_kernel(keep_ref, got_ref, coef_ref, out_ref):
    n, rows, _ = keep_ref.shape
    xh = lax.axis_index("xh")
    parts = [ref[y].astype(F32) for ref in (keep_ref, got_ref) for y in range(n)]
    lhs = jnp.concatenate(parts, axis=0).astype(BF16)
    out = jnp.dot(lhs, coef_ref[...], preferred_element_type=F32)
    count = out.shape[1]
    for i in range(2 * n):
        part = out[i * rows : (i + 1) * rows].astype(BF16)
        orbital = 2 * (i % n) + (xh if i < n else 1 - xh)
        out_ref[:, pl.ds(pl.multiple_of(orbital * count, 128), count)] = part


def work(metric, amplitudes, virt_coef):
    rows, cols = amplitudes.shape
    half, width = rows // 2, metric.shape[1]
    by_core = pl.pallas_call(
        split_kernel,
        in_specs=[VMEM],
        out_specs=VMEM,
        out_shape=jax.ShapeDtypeStruct((8, 2, half, width), BF16),
        compiler_params=PARAMS,
    )(pltpu.with_memory_space_constraint(metric, pltpu.HBM))
    ys = exchange(by_core.reshape(16, half, width), ("y", "c"))
    wanted = pl.pallas_call(
        twice_kernel,
        in_specs=[VMEM],
        out_specs=VMEM,
        out_shape=jax.ShapeDtypeStruct((2, 2, 4, 2, half, width), BF16),
        compiler_params=PARAMS,
    )(ys.reshape(2, 4, 2, half, width))
    part = exchange(wanted.reshape(4, 4, 2, half, width), ("xl", "xh"))
    part = part.reshape(2, 2, 4, 2, half, width)

    got = shifted(amplitudes, "c", 1)
    packed = pl.pallas_call(
        pack_kernel,
        in_specs=[VMEM] * 2,
        out_specs=VMEM,
        out_shape=pltpu.VMEM((rows, 2 * cols), BF16),
        compiler_params=PARAMS,
    )(
        pltpu.with_memory_space_constraint(amplitudes, pltpu.HBM),
        pltpu.with_memory_space_constraint(got, pltpu.VMEM),
    )
    steps = [packed]
    for _ in range(1, 4):
        steps.append(ring_step(steps[-1]))
    swaps = [shifted(steps[s], "c", 1) for s in range(1, 4)]
    steps.append(ring_step(steps[3]))
    shape = (half, 2 * cols)

    def on_blocks(kernel, outs, scratch, *args):
        spaces = [pltpu.HBM if a.dtype == F32 else pltpu.VMEM for a in args] + [pltpu.VMEM] * 5 + [pltpu.HBM] * 3
        args = list(map(pltpu.with_memory_space_constraint, (*args, *steps, *swaps), spaces))
        return pl.pallas_call(
            kernel,
            in_specs=[VMEM] * len(args),
            out_specs=[VMEM] * len(outs),
            out_shape=[space(shape, dtype) for space, shape, dtype in outs],
            scratch_shapes=scratch,
            compiler_params=PARAMS,
        )(*args)

    own, other, own_sent, other_sent = on_blocks(
        fitted_kernel,
        [(pltpu.VMEM, shape, F32), (pltpu.HBM, shape, F32)] + [(pltpu.VMEM, shape, BF16)] * 2,
        [],
        part,
    )
    own_arrived = shifted(other_sent, "xl", 1)
    other_arrived = shifted(own_sent, "xl", 1)
    (fitted,) = in_vmem(join_kernel, [(shape, BF16)], own, own_arrived)
    piece = (4, 2, half, half)
    slots = on_blocks(
        density_kernel,
        [(pltpu.VMEM, piece, BF16)] * 4,
        [pltpu.VMEM((4, *piece), BF16)],
        fitted, other, other_arrived,
    )
    arrived = [shifted_x(slots[s], s) for s in (2, 3, 1)]
    (xs,) = in_vmem(half_sum_kernel, [((8, 2, half, half), BF16)], slots[0], *arrived)
    got = exchange(xs.reshape(16, half, half), ("y", "c"))
    density = pl.pallas_call(
        last_sum_kernel,
        in_specs=[VMEM],
        out_specs=VMEM,
        out_shape=jax.ShapeDtypeStruct((rows // 16, 2, 8, half), F32),
        compiler_params=PARAMS,
    )(got.reshape(8, 2, half, half))

    got = exchange(fitted.reshape(8, 2, 8, 2 * cols), "y")
    kept, sent = in_vmem(pick_kernel, [((8, 8, 2 * cols), BF16)] * 2, got)
    came = shifted(sent, "xh", 1)
    ao_count = virt_coef.shape[1]
    ao = pl.pallas_call(
        ao_kernel,
        in_specs=[VMEM] * 3,
        out_specs=VMEM,
        out_shape=jax.ShapeDtypeStruct((8, 16 * ao_count), BF16),
        compiler_params=PARAMS,
    )(kept, came, pltpu.with_memory_space_constraint(virt_coef, pltpu.HBM))
    return density.reshape(rows, half), ao


def solution(mesh):
    split = Mesh(mesh.devices.reshape(2, 8, 8, 2, 2), ALL)
    return jax.shard_map(
        work,
        mesh=split,
        in_specs=(P(AUX, PAIR), P(AUX, PAIR), P()),
        out_specs=(P(AUX, PAIR), P(ALL, None)),
        check_vma=False,
    )
```

```python
import jax
import jax.numpy as jnp
from jax import lax
from jax.experimental import pallas as pl
from jax.experimental.pallas import tpu as pltpu
from jax.sharding import Mesh
from jax.sharding import PartitionSpec as P


AUX = ("xl", "z")
PAIR = ("y", "xh", "c")
ALL = AUX + PAIR
VMEM = pl.BlockSpec(memory_space=pltpu.VMEM)
PARAMS = pltpu.CompilerParams(vmem_limit_bytes=24 * 1024 * 1024)
F32, BF16 = jnp.float32, jnp.bfloat16


def in_vmem(kernel, outs, *args):
    args = [pltpu.with_memory_space_constraint(a, pltpu.VMEM) for a in args]
    return pl.pallas_call(
        kernel,
        in_specs=[VMEM] * len(args),
        out_specs=[VMEM] * len(outs),
        out_shape=[pltpu.VMEM(shape, dtype) for shape, dtype in outs],
        compiler_params=PARAMS,
    )(*args)


def shifted(x, axis, by):
    n = lax.axis_size(axis)
    return lax.ppermute(x, axis, [(i, (i + by) % n) for i in range(n)])


def exchange(x, axes):
    return lax.all_to_all(x, axes, split_axis=0, concat_axis=0, tiled=True)


def ring_step(x):
    n = lax.axis_size("z")
    moves = [(2 * i, 2 * ((i + 1) % n)) for i in range(n)]
    moves += [(2 * i + 1, 2 * ((i - 1) % n) + 1) for i in range(n)]
    return lax.ppermute(x, ("z", "c"), moves)


def shifted_x(x, by):
    at = lambda i: (i % 2) * 2 + i // 2
    return lax.ppermute(x, ("xl", "xh"), [(at(i), at((i + by) % 4)) for i in range(4)])


def blocks_of(refs):
    toward = 2 * lax.axis_index("c") - 1
    near = [(toward * s, ref[...]) for s, ref in enumerate(refs[:5])]
    return near + [(-toward * (i + 1), ref[...]) for i, ref in enumerate(refs[5:])]


def place(offset):
    at = lax.rem(lax.axis_index("z") + offset + 8, 8)
    return lax.rem(at, 2), lax.div(at, 2)


def twice_kernel(in_ref, out_ref):
    for h in range(2):
        for i in range(2):
            out_ref[h, i] = in_ref[h]


def pack_kernel(amp_ref, got_ref, out_ref):
    cols = got_ref.shape[1]
    first = lax.axis_index("c") == 0
    own, got = amp_ref[...], got_ref[...]
    out_ref[:, :cols] = jnp.where(first, own, got)
    out_ref[:, cols:] = jnp.where(first, got, own)


def split_kernel(in_ref, out_ref):
    n, cores, rows, cols = out_ref.shape
    groups = in_ref[...].astype(F32).reshape(rows // 8, cores, 8, cols)
    for c in range(cores):
        part = groups[:, c].reshape(rows, cols).astype(BF16)
        for i in range(n):
            out_ref[i, c] = part


def fitted_kernel(metric_ref, *refs):
    blocks = blocks_of(refs[:8])
    wide_refs, narrow_refs = refs[8:10], refs[10:12]
    xl = lax.axis_index("xl")
    rhs = jnp.concatenate([b for _, b in blocks], axis=0)
    lhs = [
        jnp.concatenate([metric_ref[(h, *place(o), j)] for o, _ in blocks for j in range(2)], axis=1)
        for h in (xl, 1 - xl)
    ]
    out = jnp.dot(jnp.concatenate(lhs, axis=0), rhs, preferred_element_type=F32)
    rows = out.shape[0] // 2
    for i in range(2):
        part = out[i * rows : (i + 1) * rows]
        wide_refs[i][...] = part
        narrow_refs[i][...] = part.astype(BF16)


def join_kernel(own_ref, arrived_ref, out_ref):
    out_ref[...] = (own_ref[...] + arrived_ref[...].astype(F32)).astype(BF16)


def density_kernel(own_ref, other_ref, arrived_ref, *refs):
    blocks, outs, all_ref = blocks_of(refs[:8]), refs[8:12], refs[12]
    xl = lax.axis_index("xl")
    x = 2 * lax.axis_index("xh") + xl
    other = (other_ref[...] + arrived_ref[...].astype(F32)).astype(BF16)
    fitted = jnp.concatenate([own_ref[...], other], axis=0)
    rows = own_ref.shape[0]
    amp = jnp.concatenate([b for _, b in blocks], axis=0)
    whole = lax.dot_general(amp, fitted, (((1,), (1,)), ((), ())), preferred_element_type=F32)
    height = blocks[0][1].shape[0]
    half = height // 2
    for i, (offset, _) in enumerate(blocks):
        out = whole[i * height : (i + 1) * height].astype(BF16)
        far, near = place(offset)
        for h, part in ((xl, out[:, :rows]), (1 - xl, out[:, rows:])):
            slot = lax.rem(2 * far + h + 4 - x, 4)
            for j in range(2):
                all_ref[slot, near, j] = part[j * half : (j + 1) * half]
    for s in range(4):
        outs[s][...] = all_ref[s]


def half_sum_kernel(here_ref, far_ref, left_ref, right_ref, out_ref):
    xl = lax.axis_index("xl")
    n = here_ref.shape[0]
    ours = here_ref[...].astype(F32) + far_ref[...].astype(F32)
    theirs = left_ref[...].astype(F32) + right_ref[...].astype(F32)
    out_ref[pl.ds(xl * n, n)] = ours.astype(BF16)
    out_ref[pl.ds((1 - xl) * n, n)] = theirs.astype(BF16)


def last_sum_kernel(in_ref, out_ref):
    groups, _, rows, _ = out_ref.shape
    for c in range(2):
        total = in_ref[0, c].astype(F32)
        for y in range(1, in_ref.shape[0]):
            total += in_ref[y, c].astype(F32)
        total = total.T
        for g in range(groups):
            out_ref[g, c] = total[g * rows : (g + 1) * rows]


def ao_kernel(got_ref, coef_ref, out_ref):
    n, rows, _ = got_ref.shape
    lhs = jnp.concatenate([got_ref[i].astype(F32) for i in range(n)], axis=0).astype(BF16)
    out = jnp.dot(lhs, coef_ref[...], preferred_element_type=F32)
    count = out.shape[1]
    for i in range(n):
        part = out[i * rows : (i + 1) * rows].astype(BF16)
        out_ref[:, i * count : (i + 1) * count] = part


def work(metric, amplitudes, virt_coef):
    rows, cols = amplitudes.shape
    half, width = rows // 2, metric.shape[1]
    by_core = pl.pallas_call(
        split_kernel,
        in_specs=[VMEM],
        out_specs=VMEM,
        out_shape=jax.ShapeDtypeStruct((8, 2, half, width), BF16),
        compiler_params=PARAMS,
    )(pltpu.with_memory_space_constraint(metric, pltpu.HBM))
    ys = exchange(by_core.reshape(16, half, width), ("y", "c"))
    wanted = pl.pallas_call(
        twice_kernel,
        in_specs=[VMEM],
        out_specs=VMEM,
        out_shape=jax.ShapeDtypeStruct((2, 2, 4, 2, half, width), BF16),
        compiler_params=PARAMS,
    )(ys.reshape(2, 4, 2, half, width))
    part = exchange(wanted.reshape(4, 4, 2, half, width), ("xl", "xh"))
    part = part.reshape(2, 2, 4, 2, half, width)

    got = shifted(amplitudes, "c", 1)
    packed = pl.pallas_call(
        pack_kernel,
        in_specs=[VMEM] * 2,
        out_specs=VMEM,
        out_shape=pltpu.VMEM((rows, 2 * cols), BF16),
        compiler_params=PARAMS,
    )(
        pltpu.with_memory_space_constraint(amplitudes, pltpu.HBM),
        pltpu.with_memory_space_constraint(got, pltpu.VMEM),
    )
    steps = [packed]
    for _ in range(1, 4):
        steps.append(ring_step(steps[-1]))
    swaps = [shifted(steps[s], "c", 1) for s in range(1, 4)]
    steps.append(ring_step(steps[3]))
    shape = (half, 2 * cols)

    def on_blocks(kernel, outs, scratch, *args):
        spaces = [pltpu.HBM if a.dtype == F32 else pltpu.VMEM for a in args] + [pltpu.VMEM] * 5 + [pltpu.HBM] * 3
        args = list(map(pltpu.with_memory_space_constraint, (*args, *steps, *swaps), spaces))
        return pl.pallas_call(
            kernel,
            in_specs=[VMEM] * len(args),
            out_specs=[VMEM] * len(outs),
            out_shape=[space(shape, dtype) for space, shape, dtype in outs],
            scratch_shapes=scratch,
            compiler_params=PARAMS,
        )(*args)

    own, other, own_sent, other_sent = on_blocks(
        fitted_kernel,
        [(pltpu.VMEM, shape, F32), (pltpu.HBM, shape, F32)] + [(pltpu.VMEM, shape, BF16)] * 2,
        [],
        part,
    )
    own_arrived = shifted(other_sent, "xl", 1)
    other_arrived = shifted(own_sent, "xl", 1)
    (fitted,) = in_vmem(join_kernel, [(shape, BF16)], own, own_arrived)
    piece = (4, 2, half, half)
    slots = on_blocks(
        density_kernel,
        [(pltpu.HBM, piece, BF16)] * 4,
        [pltpu.VMEM((4, *piece), BF16)],
        fitted, other, other_arrived,
    )
    arrived = [shifted_x(slots[s], s) for s in (2, 3, 1)]
    (xs,) = in_vmem(half_sum_kernel, [((8, 2, half, half), BF16)], slots[0], *arrived)
    got = exchange(xs.reshape(16, half, half), ("y", "c"))
    density = pl.pallas_call(
        last_sum_kernel,
        in_specs=[VMEM],
        out_specs=VMEM,
        out_shape=jax.ShapeDtypeStruct((rows // 16, 2, 8, half), F32),
        compiler_params=PARAMS,
    )(got.reshape(8, 2, half, half))

    got = exchange(fitted.reshape(16, 8, 2 * cols), ("y", "xh"))
    ao_count = virt_coef.shape[1]
    ao = pl.pallas_call(
        ao_kernel,
        in_specs=[VMEM] * 2,
        out_specs=VMEM,
        out_shape=jax.ShapeDtypeStruct((8, 16 * ao_count), BF16),
        compiler_params=PARAMS,
    )(got, pltpu.with_memory_space_constraint(virt_coef, pltpu.HBM))
    return density.reshape(rows, half), ao


def solution(mesh):
    split = Mesh(mesh.devices.reshape(2, 8, 8, 2, 2), ALL)
    return jax.shard_map(
        work,
        mesh=split,
        in_specs=(P(AUX, PAIR), P(AUX, PAIR), P()),
        out_specs=(P(AUX, PAIR), P(ALL, None)),
        check_vma=False,
    )
```
